128 devices in a mesh: dom: 128 (over z, y, x, core).
Axes of the slice: x: 4, y: 4, z: 4, core: 2. Of those that a mesh axis runs over, the one named last changes fastest.
Arguments:
- right_side: float32 [18, 131072], P(None, 'dom'), may hold values from -20 to 20
- element_matrix: bfloat16 [72, 72, 65536], P(None, None, 'dom'), may hold values from -8 to 8, as said below
- face_map: int32 [4, 65536], P(None, 'dom'), may hold values from 0 to 1535
- share_index: int32 [128, 4, 128], P('dom'), may hold values from 0 to 1023
- share_count: int32 [128, 4], P('dom'), may hold values from 0 to 128, as said below
- face_mass: float32 [131072], P('dom'), may hold values from 0.5 to 2
- absorbing: int32 [131072], P('dom'), may hold values 0 or 1
- impedance: float32 [131072], P('dom'), may hold values from 0.5 to 4
Outputs:
- solution: float32 [18, 131072], P(None, 'dom')
- residual: float32 [18, 131072], P(None, 'dom')
The draws below stay inside these ranges and needn't reach their ends.
Inputs may be any that keep to these rules, and one draw needn't show every extreme that they name: `element_matrix`: each element's 72 x 72 matrix is symmetric positive definite. share_count[d, k] is 0 where device d + o_k lies outside the axis; it equals 128 for some device and offset in every draw.
All inputs are finite; a program needn't handle non-finite values. No bound on the sum of `absorbing` on one device may be relied on, other than what follows from the above.
Results may differ from the reference program's by a relative error of at most 0.0003.
Values sent between devices are 32-bit elements; how exact they have to be, the bound alone decides.
No kernel may reach another device: no remote copies, remote signals or barrier semaphores. Data moves between devices by JAX's collectives and lax.ppermute only.
A program may use at most 64 MiB of HBM per device.

```python
import math
import jax
import jax.numpy as jnp
from jax import lax

TRACE = 18
SIDES = 4
DOFS = 72
REACH = 2
OFFSETS = 4
E_DEV = 512
F_DEV = 1024
GH = 128
ITERS = 2
E_TOTAL = 65536
F_TOTAL = 131072
N_DOM = 128


def draw_right_side(key, part):
    devices = F_TOTAL // F_DEV
    first_key, second_key, third_key = jax.random.split(key, 3)
    base_draw = jnp.clip(jax.random.normal(first_key, (TRACE, F_TOTAL), jnp.float32), -4.0, 4.0)
    component = jnp.exp(jax.random.uniform(second_key, (TRACE,), jnp.float32, jnp.log(0.5), jnp.log(5.0)))
    face_scale = jnp.exp(jax.random.uniform(third_key, (F_TOTAL,), jnp.float32, jnp.log(0.3), jnp.log(3.0)))
    device_of = jnp.arange(F_TOTAL, dtype=jnp.int32) // F_DEV
    ramp_scale = jnp.power(3.0, 0.5 * device_of.astype(jnp.float32) / (devices - 1))
    values_out = base_draw * component[:, None] * face_scale[None, :] * ramp_scale[None, :] * 0.25
    return jnp.clip(values_out, -20.0, 20.0).astype(jnp.float32)


def draw_element_matrix(key, part):
    devices = E_TOTAL // E_DEV

    def one_device(part_index):
        device_key = jax.random.fold_in(key, part_index)
        first_key, second_key = jax.random.split(device_key)
        raw_draw = jnp.clip(jax.random.normal(first_key, (DOFS, DOFS, E_DEV), jnp.float32), -5.0, 5.0)
        symmetric = 0.5 * (raw_draw + raw_draw.transpose(1, 0, 2)) * 0.025
        identity = jnp.eye(DOFS, dtype=jnp.float32)[:, :, None]
        off_diag = symmetric * (1.0 - identity)
        rowsum = jnp.sum(jnp.abs(off_diag), axis=1)
        stiffness = jnp.exp(jax.random.uniform(second_key, (E_DEV,), jnp.float32, jnp.log(0.5), jnp.log(2.0)))
        matrix = (off_diag + identity * (rowsum + 0.3)[:, None, :]) * stiffness[None, None, :]
        return matrix.astype(jnp.bfloat16)
    stacked = lax.map(one_device, jnp.arange(devices, dtype=jnp.int32))
    return jnp.moveaxis(stacked, 0, 2).reshape(DOFS, DOFS, E_TOTAL)


def draw_share_count(key, part):
    devices = F_TOTAL // F_DEV
    first_key, second_key, third_key, fourth_key = jax.random.split(key, 4)
    full_draw = jax.random.randint(first_key, (devices, OFFSETS), 0, 4)
    small_draw = jax.random.randint(second_key, (devices, OFFSETS), 0, GH // 4 + 1)
    counts = jnp.where(full_draw == 0, GH, small_draw)
    row_index = lax.broadcasted_iota(jnp.int32, (devices, OFFSETS), 0)
    blocks = lax.broadcasted_iota(jnp.int32, (devices, OFFSETS), 1)
    shift_by = jnp.where(blocks < REACH, blocks - REACH, blocks - REACH + 1)
    inside = (row_index + shift_by >= 0) & (row_index + shift_by < devices)
    pick_row = jax.random.randint(third_key, (), REACH, devices - REACH)
    pick_block = jax.random.randint(fourth_key, (), 0, OFFSETS)
    counts = jnp.where((row_index == pick_row) & (blocks == pick_block), GH, counts)
    return jnp.where(inside, counts, 0).astype(jnp.int32)


def touch_ends(entries, rng, smallest, top_value):
    shape = entries.shape
    index_at = [jax.random.randint(jax.random.fold_in(rng, axis), (), 0, shape[axis]) for axis in range(len(shape))]
    entries = entries.at[tuple(index_at)].set(smallest)
    longest = shape.index(max(shape))
    index_at[longest] = (index_at[longest] + 1) % shape[longest]
    return entries.at[tuple(index_at)].set(top_value)


def level_of(rng, shape, cuts, low, top_value):
    factor_of, own = 1.0, jax.random.fold_in(rng, 6)
    for axis_at, shards_of in cuts:
        heights = jnp.exp(jax.random.uniform(jax.random.fold_in(own, axis_at), (shards_of,), jnp.float32, low / len(cuts), top_value / len(cuts)))
        factor_of = factor_of * jnp.repeat(heights, shape[axis_at] // shards_of).reshape([-1 if axis == axis_at else 1 for axis in range(len(shape))])
    return factor_of


def setup_inputs(seed: int = 0) -> dict:
    streams_of = jax.random.split(jax.random.key(seed), 9)
    right_side = draw_right_side(jax.random.fold_in(streams_of[8], 71), 0)
    element_matrix = draw_element_matrix(jax.random.fold_in(streams_of[8], 71), 0)
    face_map = touch_ends(jax.random.randint(streams_of[2], (SIDES, E_TOTAL), 0, F_DEV + OFFSETS * GH), jax.random.fold_in(streams_of[2], 1), 0, (F_DEV + OFFSETS * GH) - 1).astype(jnp.int32)
    share_index = touch_ends(jax.random.randint(streams_of[3], (N_DOM, OFFSETS, GH), 0, F_DEV), jax.random.fold_in(streams_of[3], 1), 0, F_DEV - 1).astype(jnp.int32)
    share_count = draw_share_count(jax.random.fold_in(streams_of[8], 71), 0)
    face_mass = jnp.clip(jnp.exp(math.log(2.0) - 1.3862944 * jax.random.uniform(streams_of[5], (F_TOTAL,), jnp.float32) ** level_of(streams_of[5], (F_TOTAL,), ((0, 128),), -0.2, 0.2)), 0.5, 2.0)
    absorbing = touch_ends((jax.random.randint(streams_of[6], (F_TOTAL,), 0, 4) < 1).astype(jnp.int32), jax.random.fold_in(streams_of[6], 1), 0, 1)
    impedance = jnp.clip(jnp.exp(math.log(4.0) - 2.0794415 * jax.random.uniform(streams_of[7], (F_TOTAL,), jnp.float32) ** level_of(streams_of[7], (F_TOTAL,), ((0, 128),), -0.2, 0.2)), 0.5, 4.0)
    return {"right_side": right_side, "element_matrix": element_matrix, "face_map": face_map, "share_index": share_index, "share_count": share_count, "face_mass": face_mass, "absorbing": absorbing, "impedance": impedance}


def offset_of(block_index):
    return block_index - REACH if block_index < REACH else block_index - REACH + 1


def slot_map(face_map, share_index, share_count):
    element_count = face_map.shape[1]
    owner = jnp.arange(element_count, dtype=jnp.int32) // E_DEV
    owner = jnp.broadcast_to(owner[None, :], face_map.shape)
    local_face = face_map < F_DEV
    ghost_slot = jnp.maximum(face_map - F_DEV, 0)
    block_index = ghost_slot // GH
    within = ghost_slot % GH
    offsets = jnp.array([offset_of(b) for b in range(OFFSETS)], dtype=jnp.int32)
    sender = owner - offsets[block_index]
    sender_ok = (sender >= 0) & (sender < N_DOM)
    sender_safe = jnp.clip(sender, 0, N_DOM - 1).astype(jnp.int32)
    remote = share_index[sender_safe, block_index, within]
    live_count = share_count[sender_safe, block_index]
    alive_slot = sender_ok & (within < live_count)
    target = jnp.where(local_face, owner * F_DEV + face_map, sender_safe * F_DEV + remote).astype(jnp.int32)
    weight = jnp.where(local_face | alive_slot, 1.0, 0.0).astype(jnp.float32)
    return target, weight


def operate(field_now, element_matrix, target, weight, diagonal):
    picked = field_now[:, target] * weight[None, :, :]
    picked = picked.transpose(1, 0, 2).reshape(DOFS, E_TOTAL)

    def one_part(part_index):
        first_element = part_index * E_DEV
        matrices = lax.dynamic_slice_in_dim(element_matrix, first_element, E_DEV, 2).astype(jnp.float32)
        traces_in = lax.dynamic_slice_in_dim(picked, first_element, E_DEV, 1)
        return jnp.sum(matrices * traces_in[None, :, :], axis=1)

    products = lax.map(one_part, jnp.arange(N_DOM, dtype=jnp.int32))
    product = products.transpose(1, 0, 2).reshape(DOFS, E_TOTAL)
    spread = product.reshape(SIDES, TRACE, E_TOTAL) * weight[:, None, :]
    spread = spread.transpose(1, 0, 2)
    result = jnp.zeros_like(field_now).at[:, target].add(spread)
    return result + diagonal[None, :] * field_now


def reference(right_side, element_matrix, face_map, share_index, share_count, face_mass, absorbing, impedance):
    diagonal = face_mass + absorbing.astype(jnp.float32) * impedance
    target, weight = slot_map(face_map, share_index, share_count)
    solution = jnp.zeros_like(right_side)
    residual = right_side
    direction = right_side
    norm_now = jnp.sum(residual * residual)
    for rounds in range(ITERS):
        image_vec = operate(direction, element_matrix, target, weight, diagonal)
        step_size = norm_now / jnp.sum(direction * image_vec)
        solution = solution + step_size * direction
        residual = residual - step_size * image_vec
        norm_next = jnp.sum(residual * residual)
        direction = residual + (norm_next / norm_now) * direction
        norm_now = norm_next
    return solution, residual
```

```python
import functools

import jax
import jax.numpy as jnp
from jax import lax
from jax.experimental import pallas as pl
from jax.experimental.pallas import tpu as pltpu
from jax.sharding import Mesh
from jax.sharding import PartitionSpec as P

DOM = "dom"
TR = 18
TP = 24
SIDES = 4
E = 512
F = 1024
GH = 128
NB = 4
SLOTS = F + NB * GH
PICKS = SIDES * E
DOFS = SIDES * TR
F32 = jnp.float32
BF16 = jnp.bfloat16
VMEM = pltpu.VMEM
SMEM = pltpu.SMEM
PARAMS = pltpu.CompilerParams(vmem_limit_bytes=60 * 1024 * 1024)


def vspec():
    return pl.BlockSpec(memory_space=VMEM)


def sspec():
    return pl.BlockSpec(memory_space=SMEM)


def pieces(x):
    hi = x.astype(BF16).astype(F32)
    rest = x - hi
    mid = rest.astype(BF16).astype(F32)
    return jnp.concatenate([hi, mid, rest - mid], axis=0).astype(BF16)


def joined(y):
    rows = y.shape[0] // 3
    return y[:rows] + y[rows : 2 * rows] + y[2 * rows :]


def pick(x, selector):
    return joined(jnp.dot(pieces(x), selector, preferred_element_type=F32))


def spread_out(x, selector):
    return joined(
        lax.dot_general(pieces(x), selector, (((1,), (1,)), ((), ())), preferred_element_type=F32)
    )


def share_selector(index_ref, count_ref):
    cols = []
    for k in range(NB):
        rows = lax.broadcasted_iota(jnp.int32, (F, GH), 0)
        lanes = lax.broadcasted_iota(jnp.int32, (1, GH), 1)
        face = jnp.where(lanes < count_ref[0, k], index_ref[k : k + 1, :], -1)
        cols.append(jnp.where(rows == face, 1.0, 0.0).astype(BF16))
    return jnp.concatenate(cols, axis=1)


def write_blocks(blocks, core, up_ref, down_ref, mid_ref):
    up_ref[0] = blocks[3][:TR]
    up_ref[1] = blocks[2][:TR]
    down_ref[0] = blocks[0][:TR]
    down_ref[1] = blocks[1][:TR]
    mid_ref[...] = jnp.where(core == 1, blocks[1][:TR], blocks[2][:TR])


def read_blocks(core, up_ref, down_ref, mid_ref):
    first, second = mid_ref[0], mid_ref[1]
    return [
        down_ref[0],
        jnp.where(core == 1, second, first),
        jnp.where(core == 1, first, second),
        up_ref[0],
    ]


def lanes_of(values):
    lane = lax.broadcasted_iota(jnp.int32, (1, GH), 1)
    row = jnp.zeros((1, GH), F32)
    for at, value in enumerate(values):
        row = row + jnp.where(lane == at, value, 0.0)
    return row


def total(x):
    return jnp.sum(jnp.sum(x, axis=0, keepdims=True), axis=1, keepdims=True)


def send_kernel(core_ref, count_ref, field_ref, index_ref, up_ref, down_ref, mid_ref, pad_ref):
    pad_ref[...] = jnp.zeros_like(pad_ref)
    pad_ref[:TR, :] = field_ref[...]
    out = pick(pad_ref[...], share_selector(index_ref, count_ref))
    blocks = [out[:, k * GH : (k + 1) * GH] for k in range(NB)]
    write_blocks(blocks, core_ref[0], up_ref, down_ref, mid_ref)


def selector_kernel(map_ref, sel_ref):
    for s in range(SIDES):
        rows = lax.broadcasted_iota(jnp.int32, (SLOTS, E), 0)
        sel_ref[:, s * E : (s + 1) * E] = jnp.where(rows == map_ref[s : s + 1, :], 1.0, 0.0).astype(BF16)


def apply_kernel(
    core_ref,
    field_ref,
    up_ref,
    down_ref,
    mid_ref,
    sel_ref,
    matrix_ref,
    own_ref,
    up_out,
    down_out,
    mid_out,
    energy_ref,
    ext_ref,
    pick_ref,
    prod_ref,
    spread_ref,
):
    core = core_ref[0]
    ext_ref[TR:, :] = jnp.zeros((TP - TR, SLOTS), F32)
    ext_ref[:TR, :F] = field_ref[...]
    for k, block in enumerate(read_blocks(core, up_ref, down_ref, mid_ref)):
        ext_ref[:TR, F + k * GH : F + (k + 1) * GH] = block
    pick_ref[...] = pick(ext_ref[...], sel_ref[...])
    for t in range(E // 128):
        acc = jnp.zeros((DOFS, 128), F32)
        for j in range(DOFS):
            s, c = divmod(j, TR)
            row = pick_ref[c : c + 1, s * E + t * 128 : s * E + (t + 1) * 128]
            acc = acc + matrix_ref[j, :, t * 128 : (t + 1) * 128].astype(F32) * row
        prod_ref[:, t * 128 : (t + 1) * 128] = acc
    spread_ref[TR:, :] = jnp.zeros((TP - TR, PICKS), F32)
    for s in range(SIDES):
        spread_ref[:TR, s * E : (s + 1) * E] = prod_ref[s * TR : (s + 1) * TR, :]
    spread = spread_ref[...]
    energy_ref[...] = lanes_of([total(spread * pick_ref[...])])
    summed = spread_out(spread, sel_ref[...])
    own_ref[...] = summed[:TR, :F]
    parts = [summed[:, F + k * GH : F + (k + 1) * GH] for k in range(NB)]
    write_blocks(parts[::-1], core, up_out, down_out, mid_out)


def finished(core, own_ref, up_ref, down_ref, mid_ref, selector, diagonal, field, back_ref):
    back_ref[...] = jnp.zeros_like(back_ref)
    for k, block in enumerate(read_blocks(core, up_ref, down_ref, mid_ref)[::-1]):
        back_ref[:TR, k * GH : (k + 1) * GH] = block
    return own_ref[...] + spread_out(back_ref[...], selector)[:TR] + diagonal * field


def diagonal_of(mass_ref, absorbing_ref, impedance_ref):
    return mass_ref[...] + absorbing_ref[...].astype(F32) * impedance_ref[...]


def combine_kernel(
    core_ref,
    count_ref,
    field_ref,
    own_ref,
    up_ref,
    down_ref,
    mid_ref,
    index_ref,
    mass_ref,
    absorbing_ref,
    impedance_ref,
    energy_ref,
    image_ref,
    up_out,
    down_out,
    mid_out,
    sums_ref,
    back_ref,
    pad_ref,
):
    core = core_ref[0]
    selector = share_selector(index_ref, count_ref)
    diagonal = diagonal_of(mass_ref, absorbing_ref, impedance_ref)
    field = field_ref[...]
    image = finished(core, own_ref, up_ref, down_ref, mid_ref, selector, diagonal, field, back_ref)
    image_ref[...] = image
    pad_ref[...] = jnp.zeros_like(pad_ref)
    pad_ref[:TR, :] = image
    out = pick(pad_ref[...], selector)
    blocks = [out[:, k * GH : (k + 1) * GH] for k in range(NB)]
    write_blocks(blocks, core, up_out, down_out, mid_out)
    sums_ref[...] = lanes_of(
        [
            total(field * field),
            total(diagonal * field * field) + energy_ref[:, :1],
            total(image * image),
            total(diagonal * image * image),
        ]
    )


def sums_kernel(sums_ref, energy_ref, out_ref):
    lane = lax.broadcasted_iota(jnp.int32, (1, GH), 1)
    row = sums_ref[...] + jnp.where(lane == 3, energy_ref[:, :1], 0.0)
    out_ref[...] = jnp.broadcast_to(row[None], out_ref.shape)


def final_kernel(
    core_ref,
    count_ref,
    field_ref,
    image_ref,
    own_ref,
    up_ref,
    down_ref,
    mid_ref,
    index_ref,
    mass_ref,
    absorbing_ref,
    impedance_ref,
    sums_ref,
    solution_ref,
    residual_ref,
    back_ref,
):
    selector = share_selector(index_ref, count_ref)
    diagonal = diagonal_of(mass_ref, absorbing_ref, impedance_ref)
    field = field_ref[...]
    image = image_ref[...]
    second = finished(
        core_ref[0], own_ref, up_ref, down_ref, mid_ref, selector, diagonal, image, back_ref
    )
    row = jnp.sum(sums_ref[...], axis=0)
    s0, s1, s2, s3 = (row[:, k : k + 1] for k in range(4))
    step0 = s0 / s1
    ratio = (step0 * step0 * s2 - s0) / s0
    grow = 1.0 + ratio
    curvature = grow * grow * s1 - 2.0 * step0 * grow * s2 + step0 * step0 * s3
    step1 = ratio * s0 / curvature
    along = step0 + step1 * grow
    solution_ref[...] = along * field - (step0 * step1) * image
    residual_ref[...] = field - along * image + (step0 * step1) * second


def shape(*dims, dtype=F32):
    return jax.ShapeDtypeStruct(dims, dtype)


BLOCKS = (shape(2, TR, GH), shape(2, TR, GH), shape(TR, GH))
PAD = VMEM((TP, F), F32)
BACK = VMEM((TP, NB * GH), F32)


def call(kernel, name, in_specs, out_shape, scratch=()):
    return pl.pallas_call(
        kernel,
        name=name,
        in_specs=in_specs,
        out_specs=jax.tree.map(lambda _: vspec(), out_shape),
        out_shape=out_shape,
        scratch_shapes=scratch,
        compiler_params=PARAMS,
    )


def shards(
    right_side, element_matrix, face_map, share_index, share_count, face_mass, absorbing, impedance
):
    count = lax.axis_size(DOM)
    core = lax.rem(lax.axis_index(DOM), 2).astype(jnp.int32)
    core_of = core.reshape(1)
    index = share_index[0]
    mass, absorb, imped = (x.reshape(1, F) for x in (face_mass, absorbing, impedance))

    def shift(value, steps):
        return lax.ppermute(value, DOM, [(i, (i + steps) % count) for i in range(count)])

    def exchange(up, down, mid):
        got_up = shift(up, 2)
        got_down = shift(down, -2)
        onward = jnp.where(core == 1, got_up[1], got_down[1])
        got_mid = lax.ppermute(jnp.stack([mid, onward]), DOM, [(i, i ^ 1) for i in range(count)])
        return got_up, got_down, got_mid

    sent = call(send_kernel, "send", [sspec(), sspec(), vspec(), vspec()], BLOCKS, [PAD])(
        core_of, share_count, right_side, index
    )
    got = exchange(*sent)
    selector = call(selector_kernel, "selector", [vspec()], shape(SLOTS, PICKS, dtype=BF16))(face_map)

    def apply_of(name, field, got):
        return call(
            apply_kernel,
            name,
            [sspec()] + [vspec()] * 6,
            (shape(TR, F),) + BLOCKS + (shape(1, GH),),
            [
                VMEM((TP, SLOTS), F32),
                VMEM((TP, PICKS), F32),
                VMEM((DOFS, E), F32),
                VMEM((TP, PICKS), F32),
            ],
        )(core_of, field, *got, selector, element_matrix)

    own, up, down, mid, energy = apply_of("apply0", right_side, got)
    back = exchange(up, down, mid)
    image, up, down, mid, sums = call(
        combine_kernel,
        "combine",
        [sspec(), sspec()] + [vspec()] * 10,
        (shape(TR, F),) + BLOCKS + (shape(1, GH),),
        [BACK, PAD],
    )(core_of, share_count, right_side, own, *back, index, mass, absorb, imped, energy)
    got = exchange(up, down, mid)
    own, up, down, mid, energy = apply_of("apply1", image, got)
    row = call(sums_kernel, "sums", [vspec(), vspec()], shape(count, 1, GH))(sums, energy)
    row = lax.all_to_all(row, DOM, 0, 0)
    back = exchange(up, down, mid)
    return call(
        final_kernel,
        "final",
        [sspec(), sspec()] + [vspec()] * 11,
        (shape(TR, F), shape(TR, F)),
        [BACK],
    )(core_of, share_count, right_side, image, own, *back, index, mass, absorb, imped, row)


def solution(mesh):
    line = P(DOM)
    in_specs = (
        P(None, DOM),
        P(None, None, DOM),
        P(None, DOM),
        P(DOM, None, None),
        P(DOM, None),
        line,
        line,
        line,
    )
    out_specs = (P(None, DOM), P(None, DOM))
    return jax.shard_map(
        shards, mesh=mesh, in_specs=in_specs, out_specs=out_specs, check_vma=False
    )
```

```python
import jax
import jax.numpy as jnp
from jax import lax
from jax.experimental import pallas as pl
from jax.experimental.pallas import tpu as pltpu
from jax.sharding import PartitionSpec as P


DOM = "dom"
TR = 18
TP = 24
SIDES = 4
E = 512
F = 1024
GH = 128
NB = 4
SHARED = NB * GH
PICKS = SIDES * E
DOFS = SIDES * TR
F32 = jnp.float32
BF16 = jnp.bfloat16
VMEM = pltpu.VMEM
SMEM = pltpu.SMEM


def pieces(x):
    hi = x.astype(BF16).astype(F32)
    rest = x - hi
    mid = rest.astype(BF16).astype(F32)
    return jnp.concatenate([hi, mid, rest - mid], axis=0).astype(BF16)


def joined(y):
    rows = y.shape[0] // 3
    return y[:rows] + y[rows : 2 * rows] + y[2 * rows :]


def pick(x, selector):
    return joined(jnp.dot(pieces(x), selector, preferred_element_type=F32))


def spread_out(x, selector):
    return joined(
        lax.dot_general(pieces(x), selector, (((1,), (1,)), ((), ())), preferred_element_type=F32)
    )


def split(x):
    return [x[:, k * GH : (k + 1) * GH] for k in range(NB)]


def write_blocks(blocks, place_ref, near_ref, far_ref, mid_ref):
    core, odd = place_ref[0], place_ref[1]
    ahead, next_up, next_down, behind = (blocks[k] for k in (3, 2, 1, 0))
    near_ref[0] = jnp.where(odd == 1, behind, ahead)
    near_ref[1] = jnp.where(odd == 1, next_down, next_up)
    far_ref[0] = jnp.where(odd == 1, ahead, behind)
    far_ref[1] = jnp.where(odd == 1, next_up, next_down)
    mid_ref[...] = jnp.where(core == 1, next_down, next_up)


def read_blocks(place_ref, near_ref, far_ref, mid_ref):
    core, odd = place_ref[0], place_ref[1]
    near, far, first, second = near_ref[0], far_ref[0], mid_ref[0], mid_ref[1]
    return [
        jnp.where(odd == 1, far, near),
        jnp.where(core == 1, second, first),
        jnp.where(core == 1, first, second),
        jnp.where(odd == 1, near, far),
    ]


def lanes_of(values):
    lane = lax.broadcasted_iota(jnp.int32, (1, GH), 1)
    row = jnp.zeros((1, GH), F32)
    for at, value in enumerate(values):
        row = row + jnp.where(lane == at, value, 0.0)
    return row


def total(x):
    return jnp.sum(jnp.sum(x, axis=0, keepdims=True), axis=1, keepdims=True)


def send_kernel(place_ref, count_ref, field_ref, index_ref, near_ref, far_ref, mid_ref, share_ref, padded_ref):
    for k in range(NB):
        rows = lax.broadcasted_iota(jnp.int32, (F, GH), 0)
        lanes = lax.broadcasted_iota(jnp.int32, (1, GH), 1)
        face = jnp.where(lanes < count_ref[0, k], index_ref[k : k + 1, :], -1)
        share_ref[:, k * GH : (k + 1) * GH] = jnp.where(rows == face, 1.0, 0.0).astype(BF16)
    padded_ref[TR:, :] = jnp.zeros((TP - TR, F), F32)
    padded_ref[:TR, :] = field_ref[...]
    write_blocks(split(pick(padded_ref[...], share_ref[...])), place_ref, near_ref, far_ref, mid_ref)


def fill_selector(map_ref, sel_ref, first):
    slots = sel_ref.shape[0]
    for s in range(SIDES):
        rows = lax.broadcasted_iota(jnp.int32, (slots, E), 0) + first
        sel_ref[:, s * E : (s + 1) * E] = jnp.where(rows == map_ref[s : s + 1, :], 1.0, 0.0).astype(BF16)


def select_kernel(map_ref, field_ref, matrix_ref, ghost_sel_ref, local_ref, held_ref, sel_ref, sem):
    copy = pltpu.make_async_copy(matrix_ref, held_ref, sem)
    copy.start()
    fill_selector(map_ref, sel_ref, 0)
    local_ref[...] = pick(field_ref[...], sel_ref[...])
    fill_selector(map_ref, ghost_sel_ref, F)
    copy.wait()


def product_kernel(place_ref, near_ref, far_ref, mid_ref, sel_ref, matrix_ref, local_ref, *refs):
    near_out, far_out, mid_out, spread_ref, pick_ref, ghost_ref, prod_ref = refs[-7:]
    for k, block in enumerate(read_blocks(place_ref, near_ref, far_ref, mid_ref)):
        ghost_ref[:, k * GH : (k + 1) * GH] = block
    pick_ref[...] = local_ref[...] + pick(ghost_ref[...], sel_ref[...])
    for t in range(E // 128):
        acc = jnp.zeros((DOFS, 128), F32)
        for j in range(DOFS):
            s, c = divmod(j, TR)
            row = pick_ref[c : c + 1, s * E + t * 128 : s * E + (t + 1) * 128]
            acc = acc + matrix_ref[j, :, t * 128 : (t + 1) * 128].astype(F32) * row
        prod_ref[:, t * 128 : (t + 1) * 128] = acc
    spread_ref[TR:, :] = jnp.zeros((TP - TR, PICKS), F32)
    for s in range(SIDES):
        spread_ref[:TR, s * E : (s + 1) * E] = prod_ref[s * TR : (s + 1) * TR, :]
    parts = split(spread_out(spread_ref[...], sel_ref[...]))
    write_blocks(parts[::-1], place_ref, near_out, far_out, mid_out)
    if len(refs) == 10:
        first_ref, second_ref, row_ref = refs[:3]
        lane = lax.broadcasted_iota(jnp.int32, (1, GH), 1)
        energy = total(spread_ref[...] * pick_ref[...])
        row = first_ref[...] + second_ref[...] + jnp.where(lane == 3, energy, 0.0)
        row_ref[...] = jnp.broadcast_to(row[None], row_ref.shape)


def diagonal_of(mass_ref, absorbing_ref, impedance_ref):
    return mass_ref[...] + absorbing_ref[...].astype(F32) * impedance_ref[...]


def own_kernel(spread_ref, map_ref, field_ref, mass_ref, absorbing_ref, impedance_ref, *refs):
    own_ref, sel_ref = refs[-2:]
    fill_selector(map_ref, sel_ref, 0)
    field = field_ref[...]
    damped = diagonal_of(mass_ref, absorbing_ref, impedance_ref) * field
    if len(refs) == 4:
        pick_ref, sums_ref = refs[:2]
        energy = total(damped * field) + total(pick_ref[...] * spread_ref[...])
        sums_ref[...] = lanes_of([total(field * field), energy])
    own_ref[...] = spread_out(spread_ref[...], sel_ref[...]) + damped


def combine_kernel(place_ref, own_ref, near_ref, far_ref, mid_ref, share_ref, image_ref, near_out, far_out, mid_out, back_ref):
    for k, block in enumerate(read_blocks(place_ref, near_ref, far_ref, mid_ref)[::-1]):
        back_ref[:, k * GH : (k + 1) * GH] = block
    image = own_ref[...] + spread_out(back_ref[...], share_ref[...])
    image_ref[...] = image
    write_blocks(split(pick(image, share_ref[...])), place_ref, near_out, far_out, mid_out)


def local_kernel(image_ref, map_ref, mass_ref, absorbing_ref, impedance_ref, local_ref, sums_ref, sel_ref):
    fill_selector(map_ref, sel_ref, 0)
    image = image_ref[...]
    local_ref[...] = pick(image, sel_ref[...])
    square = image * image
    weighted = diagonal_of(mass_ref, absorbing_ref, impedance_ref) * square
    sums_ref[...] = lanes_of([0.0, 0.0, total(square), total(weighted)])


def final_kernel(
    place_ref, own_ref, near_ref, far_ref, mid_ref, share_ref, field_ref, image_ref, sums_ref, solution_ref, residual_ref, back_ref
):
    for k, block in enumerate(read_blocks(place_ref, near_ref, far_ref, mid_ref)[::-1]):
        back_ref[:, k * GH : (k + 1) * GH] = block
    second = own_ref[...] + spread_out(back_ref[...], share_ref[...])
    field, image = field_ref[:TR], image_ref[:TR]
    row = jnp.sum(sums_ref[...], axis=0)
    s0, s1, s2, s3 = (row[:, k : k + 1] for k in range(4))
    step0 = s0 / s1
    ratio = (step0 * step0 * s2 - s0) / s0
    grow = 1.0 + ratio
    curvature = grow * grow * s1 - 2.0 * step0 * grow * s2 + step0 * step0 * s3
    step1 = ratio * s0 / curvature
    along = step0 + step1 * grow
    solution_ref[...] = along * field - (step0 * step1) * image
    residual_ref[...] = field - along * image + (step0 * step1) * second[:TR]


MESSAGE = (VMEM((2, TP, GH), F32), VMEM((2, TP, GH), F32), VMEM((TP, GH), F32))
WIDE = VMEM((TP, PICKS), F32)
FACES = VMEM((TP, F), F32)
GHOSTS = VMEM((TP, SHARED), F32)
ROW = VMEM((1, GH), F32)


OWN_SELECTOR = VMEM((F, PICKS), BF16)
ANY = pl.ANY


def call(kernel, out_shape, *args, scratch=(), scalars=1, held=VMEM, last=VMEM):
    spaces = [SMEM] * scalars + [VMEM] * (len(args) - scalars - 1) + [last]
    args = [
        a if m is SMEM else pltpu.with_memory_space_constraint(a, pltpu.HBM if m is ANY else held)
        for a, m in zip(args, spaces)
    ]
    return pl.pallas_call(
        kernel,
        in_specs=[pl.BlockSpec(memory_space=m) for m in spaces],
        out_specs=jax.tree.map(lambda _: pl.BlockSpec(memory_space=VMEM), out_shape),
        out_shape=out_shape,
        scratch_shapes=scratch,
        compiler_params=pltpu.CompilerParams(vmem_limit_bytes=16 * 1024 * 1024),
    )(*args)


def shards(
    right_side, element_matrix, face_map, share_index, share_count, face_mass, absorbing, impedance
):
    count = lax.axis_size(DOM)
    here = lax.axis_index(DOM).astype(jnp.int32)
    core, odd = here & 1, (here >> 1) & 1
    place = jnp.stack([core, odd])
    diagonal = [x.reshape(1, F) for x in (face_mass, absorbing, impedance)]
    chips = range(count // 2)
    far_of = [(((c + 1) ^ 1) - 1) % (count // 2) for c in chips]

    def swap(value, partner):
        return lax.ppermute(value, DOM, [(2 * c + b, 2 * partner[c] + b) for c in chips for b in range(2)])

    def exchange(near, far, mid, beside):
        got_far = swap(far, far_of)
        got_near = swap(near, [c ^ 1 for c in chips])
        got_near, got_far, beside = lax.optimization_barrier((got_near, got_far, beside()))
        onward = jnp.where(core == odd, got_near[1], got_far[1])
        pair = jnp.stack([mid, onward])
        got_mid = lax.ppermute(pair, DOM, [(i, i ^ 1) for i in range(count)])
        return (got_near, got_far, got_mid), beside

    *sent, share, padded = call(
        send_kernel,
        MESSAGE + (VMEM((F, SHARED), BF16), FACES),
        place,
        share_count,
        right_side,
        share_index[0],
        scalars=2,
        held=pltpu.HBM,
    )

    def select():
        return call(
            select_kernel,
            (VMEM((SHARED, PICKS), BF16), WIDE, VMEM((DOFS, DOFS, E), BF16)),
            face_map,
            padded,
            element_matrix,
            scratch=[OWN_SELECTOR, pltpu.SemaphoreType.DMA],
            scalars=0,
            last=ANY,
        )

    got, (selector, local, matrix) = exchange(*sent, select)
    scratch = [GHOSTS, VMEM((DOFS, E), F32)]
    *sent, spread, picked = call(
        product_kernel, MESSAGE + (WIDE, WIDE), place, *got, selector, matrix, local, scratch=scratch
    )

    def own0():
        return call(
            own_kernel, (ROW, FACES), spread, face_map, padded, *diagonal, picked, scratch=[OWN_SELECTOR], scalars=0
        )

    got, (sums0, own) = exchange(*sent, own0)
    image, *sent = call(combine_kernel, (FACES,) + MESSAGE, place, own, *got, share, scratch=[GHOSTS])

    def local1():
        return call(local_kernel, (WIDE, ROW), image, face_map, *diagonal, scratch=[OWN_SELECTOR], scalars=0)

    got, (local, sums1) = exchange(*sent, local1)
    row, *sent, spread = call(
        product_kernel,
        (jax.ShapeDtypeStruct((count, 1, GH), F32),) + MESSAGE + (WIDE,),
        place,
        *got,
        selector,
        matrix,
        local,
        sums0,
        sums1,
        scratch=[WIDE] + scratch,
    )
    row = lax.all_to_all(row, DOM, 0, 0)

    def own1():
        return call(own_kernel, FACES, spread, face_map, image, *diagonal, scratch=[OWN_SELECTOR], scalars=0)

    got, own = exchange(*sent, own1)
    out = jax.ShapeDtypeStruct((TR, F), F32)
    return call(final_kernel, (out, out), place, own, *got, share, padded, image, row, scratch=[GHOSTS])


def solution(mesh):
    line = P(DOM)
    in_specs = (
        P(None, DOM),
        P(None, None, DOM),
        P(None, DOM),
        P(DOM, None, None),
        P(DOM, None),
        line,
        line,
        line,
    )
    out_specs = (P(None, DOM), P(None, DOM))
    return jax.shard_map(shards, mesh=mesh, in_specs=in_specs, out_specs=out_specs, check_vma=False)
```

```python
import jax
import jax.numpy as jnp
from jax import lax
from jax.experimental import pallas as pl
from jax.experimental.pallas import tpu as pltpu
from jax.sharding import PartitionSpec as P


DOM = "dom"
TR = 18
TP = 24
SIDES = 4
E = 512
F = 1024
GH = 128
NB = 4
SHARED = NB * GH
PICKS = SIDES * E
DOFS = SIDES * TR
F32 = jnp.float32
BF16 = jnp.bfloat16
VMEM = pltpu.VMEM
SMEM = pltpu.SMEM


def pieces(x):
    hi = x.astype(BF16).astype(F32)
    rest = x - hi
    mid = rest.astype(BF16).astype(F32)
    return jnp.concatenate([hi, mid, rest - mid], axis=0).astype(BF16)


def joined(y):
    rows = y.shape[0] // 3
    return y[:rows] + y[rows : 2 * rows] + y[2 * rows :]


def pick(x, selector):
    return joined(jnp.dot(pieces(x), selector, preferred_element_type=F32))


def spread_out(x, selector):
    return joined(
        lax.dot_general(pieces(x), selector, (((1,), (1,)), ((), ())), preferred_element_type=F32)
    )


def split(x):
    return [x[:, k * GH : (k + 1) * GH] for k in range(NB)]


def write_blocks(blocks, place_ref, near_ref, far_ref, mid_ref):
    core, odd = place_ref[0], place_ref[1]
    ahead, next_up, next_down, behind = (blocks[k] for k in (3, 2, 1, 0))
    near_ref[0] = jnp.where(odd == 1, behind, ahead)
    near_ref[1] = jnp.where(odd == 1, next_down, next_up)
    far_ref[0] = jnp.where(odd == 1, ahead, behind)
    far_ref[1] = jnp.where(odd == 1, next_up, next_down)
    mid_ref[...] = jnp.where(core == 1, next_down, next_up)


def read_blocks(place_ref, near_ref, far_ref, mid_ref):
    core, odd = place_ref[0], place_ref[1]
    near, far, first, second = near_ref[0], far_ref[0], mid_ref[0], mid_ref[1]
    return [
        jnp.where(odd == 1, far, near),
        jnp.where(core == 1, second, first),
        jnp.where(core == 1, first, second),
        jnp.where(odd == 1, near, far),
    ]


def lanes_of(values):
    lane = lax.broadcasted_iota(jnp.int32, (1, GH), 1)
    row = jnp.zeros((1, GH), F32)
    for at, value in enumerate(values):
        row = row + jnp.where(lane == at, value, 0.0)
    return row


def total(x):
    return jnp.sum(jnp.sum(x, axis=0, keepdims=True), axis=1, keepdims=True)


def send_kernel(place_ref, count_ref, field_ref, index_ref, near_ref, far_ref, mid_ref, share_ref, padded_ref):
    for k in range(NB):
        rows = lax.broadcasted_iota(jnp.int32, (F, GH), 0)
        lanes = lax.broadcasted_iota(jnp.int32, (1, GH), 1)
        face = jnp.where(lanes < count_ref[:, k : k + 1], index_ref[k : k + 1, :], -1)
        share_ref[:, k * GH : (k + 1) * GH] = jnp.where(rows == face, 1.0, 0.0).astype(BF16)
    padded_ref[TR:, :] = jnp.zeros((TP - TR, F), F32)
    padded_ref[:TR, :] = field_ref[...]
    write_blocks(split(pick(padded_ref[...], share_ref[...])), place_ref, near_ref, far_ref, mid_ref)


def fill_selector(map_ref, sel_ref, first):
    slots = sel_ref.shape[0]
    for s in range(SIDES):
        rows = lax.broadcasted_iota(jnp.int32, (slots, E), 0) + first
        sel_ref[:, s * E : (s + 1) * E] = jnp.where(rows == map_ref[s : s + 1, :], 1.0, 0.0).astype(BF16)


def select_kernel(map_ref, field_ref, matrix_ref, ghost_sel_ref, local_ref, held_ref, sel_ref, sem):
    copy = pltpu.make_async_copy(matrix_ref, held_ref, sem)
    copy.start()
    fill_selector(map_ref, sel_ref, 0)
    local_ref[...] = pick(field_ref[...], sel_ref[...])
    fill_selector(map_ref, ghost_sel_ref, F)
    copy.wait()


def product_kernel(place_ref, near_ref, far_ref, mid_ref, sel_ref, matrix_ref, local_ref, *refs):
    near_out, far_out, mid_out, spread_ref, pick_ref, ghost_ref, prod_ref = refs[-7:]
    for k, block in enumerate(read_blocks(place_ref, near_ref, far_ref, mid_ref)):
        ghost_ref[:, k * GH : (k + 1) * GH] = block
    pick_ref[...] = local_ref[...] + pick(ghost_ref[...], sel_ref[...])
    for t in range(E // 128):
        acc = jnp.zeros((DOFS, 128), F32)
        for j in range(DOFS):
            s, c = divmod(j, TR)
            row = pick_ref[c : c + 1, s * E + t * 128 : s * E + (t + 1) * 128]
            acc = acc + matrix_ref[j, :, t * 128 : (t + 1) * 128].astype(F32) * row
        prod_ref[:, t * 128 : (t + 1) * 128] = acc
    spread_ref[TR:, :] = jnp.zeros((TP - TR, PICKS), F32)
    for s in range(SIDES):
        spread_ref[:TR, s * E : (s + 1) * E] = prod_ref[s * TR : (s + 1) * TR, :]
    parts = split(spread_out(spread_ref[...], sel_ref[...]))
    write_blocks(parts[::-1], place_ref, near_out, far_out, mid_out)
    if len(refs) == 10:
        first_ref, second_ref, row_ref = refs[:3]
        lane = lax.broadcasted_iota(jnp.int32, (1, GH), 1)
        energy = total(spread_ref[...] * pick_ref[...])
        row = first_ref[...] + second_ref[...] + jnp.where(lane == 3, energy, 0.0)
        row_ref[...] = jnp.broadcast_to(row[None], row_ref.shape)


def diagonal_of(mass_ref, absorbing_ref, impedance_ref):
    return mass_ref[...] + absorbing_ref[...].astype(F32) * impedance_ref[...]


def own_kernel(spread_ref, map_ref, field_ref, mass_ref, absorbing_ref, impedance_ref, *refs):
    own_ref, sel_ref = refs[-2:]
    fill_selector(map_ref, sel_ref, 0)
    field = field_ref[...]
    damped = diagonal_of(mass_ref, absorbing_ref, impedance_ref) * field
    if len(refs) == 4:
        pick_ref, sums_ref = refs[:2]
        energy = total(damped * field) + total(pick_ref[...] * spread_ref[...])
        sums_ref[...] = lanes_of([total(field * field), energy])
    own_ref[...] = spread_out(spread_ref[...], sel_ref[...]) + damped


def combine_kernel(place_ref, own_ref, near_ref, far_ref, mid_ref, share_ref, image_ref, near_out, far_out, mid_out, back_ref):
    for k, block in enumerate(read_blocks(place_ref, near_ref, far_ref, mid_ref)[::-1]):
        back_ref[:, k * GH : (k + 1) * GH] = block
    image = own_ref[...] + spread_out(back_ref[...], share_ref[...])
    image_ref[...] = image
    write_blocks(split(pick(image, share_ref[...])), place_ref, near_out, far_out, mid_out)


def local_kernel(image_ref, map_ref, mass_ref, absorbing_ref, impedance_ref, local_ref, sums_ref, sel_ref):
    fill_selector(map_ref, sel_ref, 0)
    image = image_ref[...]
    local_ref[...] = pick(image, sel_ref[...])
    square = image * image
    weighted = diagonal_of(mass_ref, absorbing_ref, impedance_ref) * square
    sums_ref[...] = lanes_of([0.0, 0.0, total(square), total(weighted)])


def final_kernel(
    place_ref, own_ref, near_ref, far_ref, mid_ref, share_ref, field_ref, image_ref, sums_ref, solution_ref, residual_ref, back_ref
):
    for k, block in enumerate(read_blocks(place_ref, near_ref, far_ref, mid_ref)[::-1]):
        back_ref[:, k * GH : (k + 1) * GH] = block
    second = own_ref[...] + spread_out(back_ref[...], share_ref[...])
    field, image = field_ref[:TR], image_ref[:TR]
    row = jnp.sum(sums_ref[...], axis=0)
    s0, s1, s2, s3 = (row[:, k : k + 1] for k in range(4))
    step0 = s0 / s1
    ratio = (step0 * step0 * s2 - s0) / s0
    grow = 1.0 + ratio
    curvature = grow * grow * s1 - 2.0 * step0 * grow * s2 + step0 * step0 * s3
    step1 = ratio * s0 / curvature
    along = step0 + step1 * grow
    solution_ref[...] = along * field - (step0 * step1) * image
    residual_ref[...] = field - along * image + (step0 * step1) * second[:TR]


MESSAGE = (VMEM((2, TP, GH), F32), VMEM((2, TP, GH), F32), VMEM((TP, GH), F32))
WIDE = VMEM((TP, PICKS), F32)
FACES = VMEM((TP, F), F32)
GHOSTS = VMEM((TP, SHARED), F32)
ROW = VMEM((1, GH), F32)


OWN_SELECTOR = VMEM((F, PICKS), BF16)
ANY = pl.ANY


def call(kernel, out_shape, *args, scratch=(), scalars=1, held=VMEM, last=VMEM):
    spaces = [SMEM] * scalars + [VMEM] * (len(args) - scalars - 1) + [last]
    args = [
        a if m is SMEM else pltpu.with_memory_space_constraint(a, pltpu.HBM if m is ANY else held)
        for a, m in zip(args, spaces)
    ]
    return pl.pallas_call(
        kernel,
        in_specs=[pl.BlockSpec(memory_space=m) for m in spaces],
        out_specs=jax.tree.map(lambda _: pl.BlockSpec(memory_space=VMEM), out_shape),
        out_shape=out_shape,
        scratch_shapes=scratch,
        compiler_params=pltpu.CompilerParams(vmem_limit_bytes=16 * 1024 * 1024),
    )(*args)


def shards(
    right_side, element_matrix, face_map, share_index, share_count, face_mass, absorbing, impedance
):
    count = lax.axis_size(DOM)
    here = lax.axis_index(DOM).astype(jnp.int32)
    core, odd = here & 1, (here >> 1) & 1
    place = jnp.stack([core, odd])
    diagonal = [x.reshape(1, F) for x in (face_mass, absorbing, impedance)]
    chips = count // 2

    def swap(value, partner_of):
        pairs = []
        for i in range(count):
            c, b = divmod(i, 2)
            partner = partner_of(c)
            pairs.append((i, 2 * partner + b if 0 <= partner < chips else i ^ 1))
        return lax.ppermute(value, DOM, pairs)

    def exchange(near, far, mid, beside):
        got_far = swap(far, lambda c: ((c + 1) ^ 1) - 1)
        got_near = swap(near, lambda c: c ^ 1)
        got_near, got_far, beside = lax.optimization_barrier((got_near, got_far, beside()))
        onward = jnp.where(core == odd, got_near[1], got_far[1])
        pair = jnp.stack([mid, onward])
        got_mid = lax.ppermute(pair, DOM, [(i, i ^ 1) for i in range(count)])
        return (got_near, got_far, got_mid), beside

    *sent, share, padded = call(
        send_kernel,
        MESSAGE + (VMEM((F, SHARED), BF16), FACES),
        place,
        share_count,
        right_side,
        share_index[0],
        held=pltpu.HBM,
    )

    def select():
        return call(
            select_kernel,
            (VMEM((SHARED, PICKS), BF16), WIDE, VMEM((DOFS, DOFS, E), BF16)),
            face_map,
            padded,
            element_matrix,
            scratch=[OWN_SELECTOR, pltpu.SemaphoreType.DMA],
            scalars=0,
            last=ANY,
        )

    got, (selector, local, matrix) = exchange(*sent, select)
    scratch = [GHOSTS, VMEM((DOFS, E), F32)]
    *sent, spread, picked = call(
        product_kernel, MESSAGE + (WIDE, WIDE), place, *got, selector, matrix, local, scratch=scratch
    )

    def own0():
        return call(
            own_kernel, (ROW, FACES), spread, face_map, padded, *diagonal, picked, scratch=[OWN_SELECTOR], scalars=0
        )

    got, (sums0, own) = exchange(*sent, own0)
    image, *sent = call(combine_kernel, (FACES,) + MESSAGE, place, own, *got, share, scratch=[GHOSTS])

    def local1():
        return call(local_kernel, (WIDE, ROW), image, face_map, *diagonal, scratch=[OWN_SELECTOR], scalars=0)

    got, (local, sums1) = exchange(*sent, local1)
    row, *sent, spread = call(
        product_kernel,
        (jax.ShapeDtypeStruct((count, 1, GH), F32),) + MESSAGE + (WIDE,),
        place,
        *got,
        selector,
        matrix,
        local,
        sums0,
        sums1,
        scratch=[WIDE] + scratch,
    )
    row = lax.all_to_all(row, DOM, 0, 0)

    def own1():
        return call(own_kernel, FACES, spread, face_map, image, *diagonal, scratch=[OWN_SELECTOR], scalars=0)

    got, own = exchange(*sent, own1)
    out = jax.ShapeDtypeStruct((TR, F), F32)
    return call(final_kernel, (out, out), place, own, *got, share, padded, image, row, scratch=[GHOSTS])


def solution(mesh):
    line = P(DOM)
    in_specs = (
        P(None, DOM),
        P(None, None, DOM),
        P(None, DOM),
        P(DOM, None, None),
        P(DOM, None),
        line,
        line,
        line,
    )
    out_specs = (P(None, DOM), P(None, DOM))
    return jax.shard_map(shards, mesh=mesh, in_specs=in_specs, out_specs=out_specs, check_vma=False)
```

```python
import jax
import jax.numpy as jnp
from jax import lax
from jax.experimental import pallas as pl
from jax.experimental.pallas import tpu as pltpu
from jax.sharding import PartitionSpec as P


DOM = "dom"
TR = 18
TP = 24
SIDES = 4
E = 512
F = 1024
GH = 128
NB = 4
SHARED = NB * GH
PICKS = SIDES * E
DOFS = SIDES * TR
F32 = jnp.float32
BF16 = jnp.bfloat16
VMEM = pltpu.VMEM


def pieces(x):
    hi = x.astype(BF16).astype(F32)
    rest = x - hi
    mid = rest.astype(BF16).astype(F32)
    return jnp.concatenate([hi, mid, rest - mid], axis=0).astype(BF16)


def joined(y):
    rows = y.shape[0] // 3
    return y[:rows] + y[rows : 2 * rows] + y[2 * rows :]


def pick(x, selector):
    return joined(jnp.dot(pieces(x), selector, preferred_element_type=F32))


def spread_out(x, selector):
    return joined(
        lax.dot_general(pieces(x), selector, (((1,), (1,)), ((), ())), preferred_element_type=F32)
    )


def place():
    here = lax.axis_index(DOM).astype(jnp.int32)
    return here & 1, (here >> 1) & 1


def split(x):
    return [x[:, k * GH : (k + 1) * GH] for k in range(NB)]


def write_blocks(blocks, near_ref, far_ref, mid_ref):
    core, odd = place()
    ahead, next_up, next_down, behind = (blocks[k] for k in (3, 2, 1, 0))
    near_ref[0] = jnp.where(odd == 1, behind, ahead)
    near_ref[1] = jnp.where(odd == 1, next_down, next_up)
    far_ref[0] = jnp.where(odd == 1, ahead, behind)
    far_ref[1] = jnp.where(odd == 1, next_up, next_down)
    mid_ref[...] = jnp.where(core == 1, next_down, next_up)


def read_blocks(near_ref, far_ref, mid_ref):
    core, odd = place()
    near, far, first, second = near_ref[0], far_ref[0], mid_ref[0], mid_ref[1]
    return [
        jnp.where(odd == 1, far, near),
        jnp.where(core == 1, second, first),
        jnp.where(core == 1, first, second),
        jnp.where(odd == 1, near, far),
    ]


def lanes_of(values):
    lane = lax.broadcasted_iota(jnp.int32, (1, GH), 1)
    row = jnp.zeros((1, GH), F32)
    for at, value in enumerate(values):
        row = row + jnp.where(lane == at, value, 0.0)
    return row


def total(x):
    return jnp.sum(jnp.sum(x, axis=0, keepdims=True), axis=1, keepdims=True)


def send_kernel(count_ref, field_ref, index_ref, near_ref, far_ref, mid_ref, share_ref, padded_ref):
    for k in range(NB):
        rows = lax.broadcasted_iota(jnp.int32, (F, GH), 0)
        lanes = lax.broadcasted_iota(jnp.int32, (1, GH), 1)
        face = jnp.where(lanes < count_ref[:, k : k + 1], index_ref[k : k + 1, :], -1)
        share_ref[:, k * GH : (k + 1) * GH] = jnp.where(rows == face, 1.0, 0.0).astype(BF16)
    padded_ref[TR:, :] = jnp.zeros((TP - TR, F), F32)
    padded_ref[:TR, :] = field_ref[...]
    write_blocks(split(pick(padded_ref[...], share_ref[...])), near_ref, far_ref, mid_ref)


def fill_selector(map_ref, sel_ref, first):
    slots = sel_ref.shape[0]
    for s in range(SIDES):
        rows = lax.broadcasted_iota(jnp.int32, (slots, E), 0) + first
        sel_ref[:, s * E : (s + 1) * E] = jnp.where(rows == map_ref[s : s + 1, :], 1.0, 0.0).astype(BF16)


def select_kernel(map_ref, field_ref, matrix_ref, ghost_sel_ref, local_ref, held_ref, sel_ref, sem):
    copy = pltpu.make_async_copy(matrix_ref, held_ref, sem)
    copy.start()
    fill_selector(map_ref, sel_ref, 0)
    local_ref[...] = pick(field_ref[...], sel_ref[...])
    fill_selector(map_ref, ghost_sel_ref, F)
    copy.wait()


def product_kernel(near_ref, far_ref, mid_ref, sel_ref, matrix_ref, local_ref, *refs):
    near_out, far_out, mid_out, spread_ref, pick_ref, ghost_ref, prod_ref = refs[-7:]
    for k, block in enumerate(read_blocks(near_ref, far_ref, mid_ref)):
        ghost_ref[:, k * GH : (k + 1) * GH] = block
    pick_ref[...] = local_ref[...] + pick(ghost_ref[...], sel_ref[...])
    for t in range(E // 128):
        acc = jnp.zeros((DOFS, 128), F32)
        for j in range(DOFS):
            s, c = divmod(j, TR)
            row = pick_ref[c : c + 1, s * E + t * 128 : s * E + (t + 1) * 128]
            acc = acc + matrix_ref[j, :, t * 128 : (t + 1) * 128].astype(F32) * row
        prod_ref[:, t * 128 : (t + 1) * 128] = acc
    spread_ref[TR:, :] = jnp.zeros((TP - TR, PICKS), F32)
    for s in range(SIDES):
        spread_ref[:TR, s * E : (s + 1) * E] = prod_ref[s * TR : (s + 1) * TR, :]
    parts = split(spread_out(spread_ref[...], sel_ref[...]))
    write_blocks(parts[::-1], near_out, far_out, mid_out)
    if len(refs) == 10:
        first_ref, second_ref, row_ref = refs[:3]
        lane = lax.broadcasted_iota(jnp.int32, (1, GH), 1)
        energy = total(spread_ref[...] * pick_ref[...])
        row = first_ref[...] + second_ref[...] + jnp.where(lane == 3, energy, 0.0)
        row_ref[...] = jnp.broadcast_to(row[None], row_ref.shape)


def diagonal_of(mass_ref, absorbing_ref, impedance_ref):
    return mass_ref[...] + absorbing_ref[...].astype(F32) * impedance_ref[...]


def own_kernel(spread_ref, map_ref, field_ref, mass_ref, absorbing_ref, impedance_ref, *refs):
    own_ref, sel_ref = refs[-2:]
    fill_selector(map_ref, sel_ref, 0)
    field = field_ref[...]
    damped = diagonal_of(mass_ref, absorbing_ref, impedance_ref) * field
    if len(refs) == 4:
        pick_ref, sums_ref = refs[:2]
        energy = total(damped * field) + total(pick_ref[...] * spread_ref[...])
        sums_ref[...] = lanes_of([total(field * field), energy])
    own_ref[...] = spread_out(spread_ref[...], sel_ref[...]) + damped


def combine_kernel(own_ref, near_ref, far_ref, mid_ref, share_ref, image_ref, near_out, far_out, mid_out, back_ref):
    for k, block in enumerate(read_blocks(near_ref, far_ref, mid_ref)[::-1]):
        back_ref[:, k * GH : (k + 1) * GH] = block
    image = own_ref[...] + spread_out(back_ref[...], share_ref[...])
    image_ref[...] = image
    write_blocks(split(pick(image, share_ref[...])), near_out, far_out, mid_out)


def local_kernel(image_ref, map_ref, mass_ref, absorbing_ref, impedance_ref, local_ref, sums_ref, sel_ref):
    fill_selector(map_ref, sel_ref, 0)
    image = image_ref[...]
    local_ref[...] = pick(image, sel_ref[...])
    square = image * image
    weighted = diagonal_of(mass_ref, absorbing_ref, impedance_ref) * square
    sums_ref[...] = lanes_of([0.0, 0.0, total(square), total(weighted)])


def final_kernel(
    own_ref, near_ref, far_ref, mid_ref, share_ref, field_ref, image_ref, sums_ref, solution_ref, residual_ref, back_ref
):
    for k, block in enumerate(read_blocks(near_ref, far_ref, mid_ref)[::-1]):
        back_ref[:, k * GH : (k + 1) * GH] = block
    second = own_ref[...] + spread_out(back_ref[...], share_ref[...])
    field, image = field_ref[:TR], image_ref[:TR]
    row = jnp.sum(sums_ref[...], axis=0)
    s0, s1, s2, s3 = (row[:, k : k + 1] for k in range(4))
    step0 = s0 / s1
    ratio = (step0 * step0 * s2 - s0) / s0
    grow = 1.0 + ratio
    curvature = grow * grow * s1 - 2.0 * step0 * grow * s2 + step0 * step0 * s3
    step1 = ratio * s0 / curvature
    along = step0 + step1 * grow
    solution_ref[...] = along * field - (step0 * step1) * image
    residual_ref[...] = field - along * image + (step0 * step1) * second[:TR]


MESSAGE = (VMEM((2, TP, GH), F32), VMEM((2, TP, GH), F32), VMEM((TP, GH), F32))
WIDE = VMEM((TP, PICKS), F32)
FACES = VMEM((TP, F), F32)
GHOSTS = VMEM((TP, SHARED), F32)
ROW = VMEM((1, GH), F32)


OWN_SELECTOR = VMEM((F, PICKS), BF16)
ANY = pl.ANY


def call(kernel, out_shape, *args, scratch=(), held=VMEM, last=VMEM):
    spaces = [VMEM] * (len(args) - 1) + [last]
    args = [pltpu.with_memory_space_constraint(a, pltpu.HBM if m is ANY else held) for a, m in zip(args, spaces)]
    return pl.pallas_call(
        kernel,
        in_specs=[pl.BlockSpec(memory_space=m) for m in spaces],
        out_specs=jax.tree.map(lambda _: pl.BlockSpec(memory_space=VMEM), out_shape),
        out_shape=out_shape,
        scratch_shapes=scratch,
        compiler_params=pltpu.CompilerParams(vmem_limit_bytes=16 * 1024 * 1024),
    )(*args)


def shards(
    right_side, element_matrix, face_map, share_index, share_count, face_mass, absorbing, impedance
):
    count = lax.axis_size(DOM)
    core, odd = place()
    diagonal = [x.reshape(1, F) for x in (face_mass, absorbing, impedance)]
    chips = count // 2

    def swap(value, partner_of):
        pairs = []
        for i in range(count):
            c, b = divmod(i, 2)
            partner = partner_of(c)
            pairs.append((i, 2 * partner + b if 0 <= partner < chips else i ^ 1))
        return lax.ppermute(value, DOM, pairs)

    def exchange(near, far, mid, beside):
        got_far = swap(far, lambda c: ((c + 1) ^ 1) - 1)
        got_near = swap(near, lambda c: c ^ 1)
        got_near, got_far, beside = lax.optimization_barrier((got_near, got_far, beside()))
        onward = jnp.where(core == odd, got_near[1], got_far[1])
        pair = jnp.stack([mid, onward])
        got_mid = lax.ppermute(pair, DOM, [(i, i ^ 1) for i in range(count)])
        return (got_near, got_far, got_mid), beside

    *sent, share, padded = call(
        send_kernel, MESSAGE + (VMEM((F, SHARED), BF16), FACES), share_count, right_side, share_index[0], held=pltpu.HBM
    )

    def select():
        return call(
            select_kernel,
            (VMEM((SHARED, PICKS), BF16), WIDE, VMEM((DOFS, DOFS, E), BF16)),
            face_map,
            padded,
            element_matrix,
            scratch=[OWN_SELECTOR, pltpu.SemaphoreType.DMA],
            last=ANY,
        )

    got, (selector, local, matrix) = exchange(*sent, select)
    scratch = [GHOSTS, VMEM((DOFS, E), F32)]
    *sent, spread, picked = call(product_kernel, MESSAGE + (WIDE, WIDE), *got, selector, matrix, local, scratch=scratch)

    def own0():
        return call(own_kernel, (ROW, FACES), spread, face_map, padded, *diagonal, picked, scratch=[OWN_SELECTOR])

    got, (sums0, own) = exchange(*sent, own0)
    image, *sent = call(combine_kernel, (FACES,) + MESSAGE, own, *got, share, scratch=[GHOSTS])

    def local1():
        return call(local_kernel, (WIDE, ROW), image, face_map, *diagonal, scratch=[OWN_SELECTOR])

    got, (local, sums1) = exchange(*sent, local1)
    row, *sent, spread = call(
        product_kernel,
        (jax.ShapeDtypeStruct((count, 1, GH), F32),) + MESSAGE + (WIDE,),
        *got,
        selector,
        matrix,
        local,
        sums0,
        sums1,
        scratch=[WIDE] + scratch,
    )
    row = lax.all_to_all(row, DOM, 0, 0)

    def own1():
        return call(own_kernel, FACES, spread, face_map, image, *diagonal, scratch=[OWN_SELECTOR])

    got, own = exchange(*sent, own1)
    out = jax.ShapeDtypeStruct((TR, F), F32)
    return call(final_kernel, (out, out), own, *got, share, padded, image, row, scratch=[GHOSTS])


def solution(mesh):
    line = P(DOM)
    in_specs = (
        P(None, DOM),
        P(None, None, DOM),
        P(None, DOM),
        P(DOM, None, None),
        P(DOM, None),
        line,
        line,
        line,
    )
    out_specs = (P(None, DOM), P(None, DOM))
    return jax.shard_map(shards, mesh=mesh, in_specs=in_specs, out_specs=out_specs, check_vma=False)
```

```python
import jax
import jax.numpy as jnp
from jax import lax
from jax.experimental import pallas as pl
from jax.experimental.pallas import tpu as pltpu
from jax.sharding import PartitionSpec as P


DOM = "dom"
TR = 18
TP = 24
SIDES = 4
E = 512
F = 1024
GH = 128
NB = 4
SHARED = NB * GH
PICKS = SIDES * E
DOFS = SIDES * TR
F32 = jnp.float32
BF16 = jnp.bfloat16
VMEM = pltpu.VMEM


def pieces(x):
    hi = x.astype(BF16).astype(F32)
    rest = x - hi
    mid = rest.astype(BF16).astype(F32)
    return jnp.concatenate([hi, mid, rest - mid], axis=0).astype(BF16)


def joined(y):
    rows = y.shape[0] // 3
    return y[:rows] + y[rows : 2 * rows] + y[2 * rows :]


def pick(x, selector):
    return joined(jnp.dot(pieces(x), selector, preferred_element_type=F32))


def spread_out(x, selector):
    return joined(
        lax.dot_general(pieces(x), selector, (((1,), (1,)), ((), ())), preferred_element_type=F32)
    )


def place():
    here = lax.axis_index(DOM).astype(jnp.int32)
    return here & 1, (here >> 1) & 1


def split(x):
    return [x[:, k * GH : (k + 1) * GH] for k in range(NB)]


def write_blocks(blocks, near_ref, far_ref, mid_ref):
    core, odd = place()
    ahead, next_up, next_down, behind = (blocks[k] for k in (3, 2, 1, 0))
    near_ref[0] = jnp.where(odd == 1, behind, ahead)
    near_ref[1] = jnp.where(odd == 1, next_down, next_up)
    far_ref[0] = jnp.where(odd == 1, ahead, behind)
    far_ref[1] = jnp.where(odd == 1, next_up, next_down)
    mid_ref[...] = jnp.where(core == 1, next_down, next_up)


def read_blocks(near_ref, far_ref, mid_ref):
    core, odd = place()
    near, far, first, second = near_ref[0], far_ref[0], mid_ref[0], mid_ref[1]
    return [
        jnp.where(odd == 1, far, near),
        jnp.where(core == 1, second, first),
        jnp.where(core == 1, first, second),
        jnp.where(odd == 1, near, far),
    ]


def lanes_of(values):
    lane = lax.broadcasted_iota(jnp.int32, (1, GH), 1)
    row = jnp.zeros((1, GH), F32)
    for at, value in enumerate(values):
        row = row + jnp.where(lane == at, value, 0.0)
    return row


def total(x):
    folded = sum(x[:, at : at + 128] for at in range(0, x.shape[1], 128))
    folded = sum(folded[at : at + 8] for at in range(0, x.shape[0], 8))
    return jnp.sum(jnp.sum(folded, axis=0, keepdims=True), axis=1, keepdims=True)


def send_kernel(count_ref, field_ref, index_ref, map_ref, mass_ref, absorbing_ref, impedance_ref, *refs):
    near_ref, far_ref, mid_ref, share_ref, padded_ref, map_out, diagonal_ref = refs
    for k in range(NB):
        rows = lax.broadcasted_iota(jnp.int32, (F, GH), 0)
        lanes = lax.broadcasted_iota(jnp.int32, (1, GH), 1)
        face = jnp.where(lanes < count_ref[:, k : k + 1], index_ref[k : k + 1, :], -1)
        share_ref[:, k * GH : (k + 1) * GH] = jnp.where(rows == face, 1.0, 0.0).astype(BF16)
    padded_ref[TR:, :] = jnp.zeros((TP - TR, F), F32)
    padded_ref[:TR, :] = field_ref[...]
    write_blocks(split(pick(padded_ref[...], share_ref[...])), near_ref, far_ref, mid_ref)
    map_out[...] = map_ref[...]
    diagonal_ref[...] = mass_ref[...] + absorbing_ref[...].astype(F32) * impedance_ref[...]


def fill_selector(map_ref, sel_ref, first):
    slots = sel_ref.shape[0]
    for s in range(SIDES):
        rows = lax.broadcasted_iota(jnp.int32, (slots, E), 0) + first
        sel_ref[:, s * E : (s + 1) * E] = jnp.where(rows == map_ref[s : s + 1, :], 1.0, 0.0).astype(BF16)


def select_kernel(map_ref, field_ref, matrix_ref, ghost_sel_ref, local_ref, wide_ref, sel_ref, held_ref, sem):
    copy = pltpu.make_async_copy(matrix_ref, held_ref, sem)
    copy.start()
    fill_selector(map_ref, sel_ref, 0)
    local_ref[...] = pick(field_ref[...], sel_ref[...])
    fill_selector(map_ref, ghost_sel_ref, F)
    copy.wait()
    for j in range(DOFS):
        for t in range(E // 128):
            wide_ref[t, j] = held_ref[j, :, t * 128 : (t + 1) * 128].astype(F32)


def product_kernel(near_ref, far_ref, mid_ref, sel_ref, matrix_ref, local_ref, *refs):
    last = len(refs) > 7
    near_out, far_out, mid_out, spread_ref, pick_ref, ghost_ref, prod_ref = refs[3:10] if last else refs
    for k, block in enumerate(read_blocks(near_ref, far_ref, mid_ref)):
        ghost_ref[:, k * GH : (k + 1) * GH] = block
    pick_ref[...] = local_ref[...] + pick(ghost_ref[...], sel_ref[...])
    for t in range(E // 128):
        acc = jnp.zeros((DOFS, 128), F32)
        for j in range(DOFS):
            s, c = divmod(j, TR)
            row = pick_ref[c : c + 1, s * E + t * 128 : s * E + (t + 1) * 128]
            acc = acc + matrix_ref[t, j] * row
        prod_ref[:, t * 128 : (t + 1) * 128] = acc
    spread_ref[TR:, :] = jnp.zeros((TP - TR, PICKS), F32)
    for s in range(SIDES):
        spread_ref[:TR, s * E : (s + 1) * E] = prod_ref[s * TR : (s + 1) * TR, :]
    if last:
        first_ref, second_ref, row_out = refs[:3]
        row_ref, sem = refs[10:]
        lane = lax.broadcasted_iota(jnp.int32, (1, GH), 1)
        energy = total(spread_ref[...] * pick_ref[...])
        row = first_ref[...] + second_ref[...] + jnp.where(lane == 3, energy, 0.0)
        row_ref[...] = jnp.broadcast_to(row[None], row_ref.shape)
        copy = pltpu.make_async_copy(row_ref, row_out, sem)
        copy.start()

    def send_back():
        parts = split(spread_out(spread_ref[...], sel_ref[...]))
        write_blocks(parts[::-1], near_out, far_out, mid_out)

    if last:
        pl.when(lax.axis_index(DOM) >= 0)(send_back)
        copy.wait()
    else:
        send_back()


def own_kernel(spread_ref, map_ref, field_ref, diagonal_ref, *refs):
    own_ref, sel_ref = refs[-2:]
    fill_selector(map_ref, sel_ref, 0)
    field = field_ref[...]
    damped = diagonal_ref[...] * field
    if len(refs) == 4:
        pick_ref, sums_ref = refs[:2]
        energy = total(damped * field) + total(pick_ref[...] * spread_ref[...])
        sums_ref[...] = lanes_of([total(field * field), energy])
    own_ref[...] = spread_out(spread_ref[...], sel_ref[...]) + damped


def combine_kernel(own_ref, near_ref, far_ref, mid_ref, share_ref, image_ref, near_out, far_out, mid_out, back_ref):
    for k, block in enumerate(read_blocks(near_ref, far_ref, mid_ref)[::-1]):
        back_ref[:, k * GH : (k + 1) * GH] = block
    image = own_ref[...] + spread_out(back_ref[...], share_ref[...])
    image_ref[...] = image
    write_blocks(split(pick(image, share_ref[...])), near_out, far_out, mid_out)


def local_kernel(image_ref, map_ref, diagonal_ref, local_ref, sums_ref, sel_ref):
    fill_selector(map_ref, sel_ref, 0)
    image = image_ref[...]
    local_ref[...] = pick(image, sel_ref[...])
    square = image * image
    weighted = diagonal_ref[...] * square
    sums_ref[...] = lanes_of([0.0, 0.0, total(square), total(weighted)])


def final_kernel(
    own_ref, near_ref, far_ref, mid_ref, share_ref, field_ref, image_ref, sums_ref, solution_ref, residual_ref, back_ref
):
    for k, block in enumerate(read_blocks(near_ref, far_ref, mid_ref)[::-1]):
        back_ref[:, k * GH : (k + 1) * GH] = block
    second = own_ref[...] + spread_out(back_ref[...], share_ref[...])
    field, image = field_ref[:TR], image_ref[:TR]
    row = jnp.sum(sums_ref[...], axis=0)
    s0, s1, s2, s3 = (row[:, k : k + 1] for k in range(4))
    step0 = s0 / s1
    ratio = (step0 * step0 * s2 - s0) / s0
    grow = 1.0 + ratio
    curvature = grow * grow * s1 - 2.0 * step0 * grow * s2 + step0 * step0 * s3
    step1 = ratio * s0 / curvature
    along = step0 + step1 * grow
    solution_ref[...] = along * field - (step0 * step1) * image
    residual_ref[...] = field - along * image + (step0 * step1) * second[:TR]


MESSAGE = (VMEM((2, TP, GH), F32), VMEM((2, TP, GH), F32), VMEM((TP, GH), F32))
WIDE = VMEM((TP, PICKS), F32)
FACES = VMEM((TP, F), F32)
GHOSTS = VMEM((TP, SHARED), F32)
ROW = VMEM((1, GH), F32)


OWN_SELECTOR = VMEM((F, PICKS), BF16)
ANY = pl.ANY


def call(kernel, out_shape, *args, scratch=(), held=VMEM, last=VMEM, first=VMEM):
    spaces = [VMEM] * (len(args) - 1) + [last]
    args = [pltpu.with_memory_space_constraint(a, pltpu.HBM if m is ANY else held) for a, m in zip(args, spaces)]
    return pl.pallas_call(
        kernel,
        in_specs=[pl.BlockSpec(memory_space=m) for m in spaces],
        out_specs=tuple(pl.BlockSpec(memory_space=VMEM if at else first) for at in range(len(out_shape))),
        out_shape=out_shape,
        scratch_shapes=scratch,
        compiler_params=pltpu.CompilerParams(vmem_limit_bytes=16 * 1024 * 1024),
    )(*args)


def shards(
    right_side, element_matrix, face_map, share_index, share_count, face_mass, absorbing, impedance
):
    count = lax.axis_size(DOM)
    core, odd = place()
    chips = count // 2

    def swap(value, partner_of):
        pairs = []
        for i in range(count):
            c, b = divmod(i, 2)
            partner = partner_of(c)
            pairs.append((i, 2 * partner + b if 0 <= partner < chips else i ^ 1))
        return lax.ppermute(value, DOM, pairs)

    def exchange(near, far, mid, beside):
        got_far = swap(far, lambda c: ((c + 1) ^ 1) - 1)
        got_near = swap(near, lambda c: c ^ 1)
        got_near, got_far, beside = lax.optimization_barrier((got_near, got_far, beside()))
        onward = jnp.where(core == odd, got_near[1], got_far[1])
        pair = jnp.stack([mid, onward])
        got_mid = lax.ppermute(pair, DOM, [(i, i ^ 1) for i in range(count)])
        return (got_near, got_far, got_mid), beside

    *sent, share, padded, held_map, diagonal = call(
        send_kernel,
        MESSAGE + (VMEM((F, SHARED), BF16), FACES, VMEM((SIDES, E), jnp.int32), VMEM((1, F), F32)),
        share_count,
        right_side,
        share_index[0],
        face_map,
        face_mass.reshape(1, F),
        absorbing.reshape(1, F),
        impedance.reshape(1, F),
        held=pltpu.HBM,
    )

    def select():
        return call(
            select_kernel,
            (VMEM((SHARED, PICKS), BF16), WIDE, VMEM((E // 128, DOFS, DOFS, 128), F32)),
            held_map,
            padded,
            element_matrix,
            scratch=[OWN_SELECTOR, VMEM((DOFS, DOFS, E), BF16), pltpu.SemaphoreType.DMA],
            last=ANY,
        )

    got, (selector, local, matrix) = exchange(*sent, select)
    scratch = [GHOSTS, VMEM((DOFS, E), F32)]
    *sent, spread, picked = call(product_kernel, MESSAGE + (WIDE, WIDE), *got, selector, matrix, local, scratch=scratch)

    def own0():
        return call(own_kernel, (ROW, FACES), spread, held_map, padded, diagonal, picked, scratch=[OWN_SELECTOR])

    got, (sums0, own) = exchange(*sent, own0)
    image, *sent = call(combine_kernel, (FACES,) + MESSAGE, own, *got, share, scratch=[GHOSTS])

    def local1():
        return call(local_kernel, (WIDE, ROW), image, held_map, diagonal, scratch=[OWN_SELECTOR])

    got, (local, sums1) = exchange(*sent, local1)
    row, *sent, spread = call(
        product_kernel,
        (jax.ShapeDtypeStruct((count, 1, GH), F32),) + MESSAGE + (WIDE,),
        *got,
        selector,
        matrix,
        local,
        sums0,
        sums1,
        scratch=[WIDE] + scratch + [VMEM((count, 1, GH), F32), pltpu.SemaphoreType.DMA],
        first=ANY,
    )
    row = lax.all_to_all(row, DOM, 0, 0)

    def own1():
        return call(own_kernel, (FACES,), spread, held_map, image, diagonal, scratch=[OWN_SELECTOR])

    got, (own,) = exchange(*sent, own1)
    out = jax.ShapeDtypeStruct((TR, F), F32)
    return call(final_kernel, (out, out), own, *got, share, padded, image, row, scratch=[GHOSTS])


def solution(mesh):
    line = P(DOM)
    in_specs = (
        P(None, DOM),
        P(None, None, DOM),
        P(None, DOM),
        P(DOM, None, None),
        P(DOM, None),
        line,
        line,
        line,
    )
    out_specs = (P(None, DOM), P(None, DOM))
    return jax.shard_map(shards, mesh=mesh, in_specs=in_specs, out_specs=out_specs, check_vma=False)
```

```python
import jax
import jax.numpy as jnp
from jax import lax
from jax.experimental import pallas as pl
from jax.experimental.pallas import tpu as pltpu
from jax.sharding import PartitionSpec as P


DOM = "dom"
TR = 18
TP = 24
SIDES = 4
E = 512
F = 1024
GH = 128
NB = 4
SHARED = NB * GH
PICKS = SIDES * E
DOFS = SIDES * TR
F32 = jnp.float32
BF16 = jnp.bfloat16
VMEM = pltpu.VMEM


def pieces(x):
    hi = x.astype(BF16).astype(F32)
    rest = x - hi
    mid = rest.astype(BF16).astype(F32)
    return jnp.concatenate([hi, mid, rest - mid], axis=0).astype(BF16)


def joined(y):
    rows = y.shape[0] // 3
    return y[:rows] + y[rows : 2 * rows] + y[2 * rows :]


def pick(x, selector):
    return joined(jnp.dot(pieces(x), selector, preferred_element_type=F32))


def spread_out(x, selector):
    return joined(
        lax.dot_general(pieces(x), selector, (((1,), (1,)), ((), ())), preferred_element_type=F32)
    )


def place():
    here = lax.axis_index(DOM).astype(jnp.int32)
    return here & 1, (here >> 1) & 1


def split(x):
    return [x[:, k * GH : (k + 1) * GH] for k in range(NB)]


def write_blocks(blocks, near_ref, far_ref, mid_ref):
    core, odd = place()
    ahead, next_up, next_down, behind = (blocks[k] for k in (3, 2, 1, 0))
    near_ref[0] = jnp.where(odd == 1, behind, ahead)
    near_ref[1] = jnp.where(odd == 1, next_down, next_up)
    far_ref[0] = jnp.where(odd == 1, ahead, behind)
    far_ref[1] = jnp.where(odd == 1, next_up, next_down)
    mid_ref[...] = jnp.where(core == 1, next_down, next_up)


def read_blocks(near_ref, far_ref, mid_ref):
    core, odd = place()
    near, far, first, second = near_ref[0], far_ref[0], mid_ref[0], mid_ref[1]
    return [
        jnp.where(odd == 1, far, near),
        jnp.where(core == 1, second, first),
        jnp.where(core == 1, first, second),
        jnp.where(odd == 1, near, far),
    ]


def quotient(a, b):
    q = a / b
    return q + (a - q * b) / b


def exact_product(a, b):
    def halves(x):
        scaled = 4097.0 * x
        high = scaled - (scaled - x)
        return high, x - high

    product = a * b
    (ah, al), (bh, bl) = halves(a), halves(b)
    return product, ((ah * bh - product) + ah * bl + al * bh) + al * bl


def determinant(a, b, c):
    (first, first_rest), (second, second_rest) = exact_product(a, c), exact_product(b, b)
    return (first - second) + (first_rest - second_rest)


def lanes_of(values):
    lane = lax.broadcasted_iota(jnp.int32, (1, GH), 1)
    row = jnp.zeros((1, GH), F32)
    for at, value in enumerate(values):
        row = row + jnp.where(lane == at, value, 0.0)
    return row


def total(x):
    folded = sum(x[:, at : at + 128] for at in range(0, x.shape[1], 128))
    folded = sum(folded[at : at + 8] for at in range(0, x.shape[0], 8))
    return jnp.sum(jnp.sum(folded, axis=0, keepdims=True), axis=1, keepdims=True)


def send_kernel(count_ref, field_ref, index_ref, map_ref, mass_ref, absorbing_ref, impedance_ref, *refs):
    near_ref, far_ref, mid_ref, share_ref, padded_ref, map_out, diagonal_ref = refs
    for k in range(NB):
        rows = lax.broadcasted_iota(jnp.int32, (F, GH), 0)
        lanes = lax.broadcasted_iota(jnp.int32, (1, GH), 1)
        face = jnp.where(lanes < count_ref[:, k : k + 1], index_ref[k : k + 1, :], -1)
        share_ref[:, k * GH : (k + 1) * GH] = jnp.where(rows == face, 1.0, 0.0).astype(BF16)
    padded_ref[TR:, :] = jnp.zeros((TP - TR, F), F32)
    padded_ref[:TR, :] = field_ref[...]
    write_blocks(split(pick(padded_ref[...], share_ref[...])), near_ref, far_ref, mid_ref)
    map_out[...] = map_ref[...]
    diagonal_ref[...] = mass_ref[...] + absorbing_ref[...].astype(F32) * impedance_ref[...]


def fill_selector(map_ref, sel_ref, first):
    slots = sel_ref.shape[0]
    for s in range(SIDES):
        rows = lax.broadcasted_iota(jnp.int32, (slots, E), 0) + first
        sel_ref[:, s * E : (s + 1) * E] = jnp.where(rows == map_ref[s : s + 1, :], 1.0, 0.0).astype(BF16)


def select_kernel(map_ref, field_ref, matrix_ref, ghost_sel_ref, local_ref, wide_ref, sel_ref, held_ref, sem):
    copy = pltpu.make_async_copy(matrix_ref, held_ref, sem)
    copy.start()
    fill_selector(map_ref, sel_ref, 0)
    local_ref[...] = pick(field_ref[...], sel_ref[...])
    fill_selector(map_ref, ghost_sel_ref, F)
    copy.wait()
    for j in range(DOFS):
        for t in range(E // 128):
            wide_ref[t, j] = held_ref[j, :, t * 128 : (t + 1) * 128].astype(F32)


def product_kernel(near_ref, far_ref, mid_ref, sel_ref, matrix_ref, local_ref, *refs):
    last = len(refs) > 7
    near_out, far_out, mid_out, spread_ref, pick_ref, ghost_ref, prod_ref = refs[3:10] if last else refs
    for k, block in enumerate(read_blocks(near_ref, far_ref, mid_ref)):
        ghost_ref[:, k * GH : (k + 1) * GH] = block
    pick_ref[...] = local_ref[...] + pick(ghost_ref[...], sel_ref[...])
    for t in range(E // 128):
        acc = jnp.zeros((DOFS, 128), F32)
        for j in range(DOFS):
            s, c = divmod(j, TR)
            row = pick_ref[c : c + 1, s * E + t * 128 : s * E + (t + 1) * 128]
            acc = acc + matrix_ref[t, j] * row
        prod_ref[:, t * 128 : (t + 1) * 128] = acc
    spread_ref[TR:, :] = jnp.zeros((TP - TR, PICKS), F32)
    for s in range(SIDES):
        spread_ref[:TR, s * E : (s + 1) * E] = prod_ref[s * TR : (s + 1) * TR, :]
    if last:
        first_ref, second_ref, row_out = refs[:3]
        row_ref, sem = refs[10:]
        lane = lax.broadcasted_iota(jnp.int32, (1, GH), 1)
        energy = total(spread_ref[...] * pick_ref[...])
        row = first_ref[...] + second_ref[...] + jnp.where(lane == 3, energy, 0.0)
        row_ref[...] = jnp.broadcast_to(row[None], row_ref.shape)
        copy = pltpu.make_async_copy(row_ref, row_out, sem)
        copy.start()

    def send_back():
        parts = split(spread_out(spread_ref[...], sel_ref[...]))
        write_blocks(parts[::-1], near_out, far_out, mid_out)

    if last:
        pl.when(lax.axis_index(DOM) >= 0)(send_back)
        copy.wait()
    else:
        send_back()


def own_kernel(spread_ref, map_ref, field_ref, diagonal_ref, *refs):
    own_ref, sel_ref = refs[-2:]
    fill_selector(map_ref, sel_ref, 0)
    field = field_ref[...]
    damped = diagonal_ref[...] * field
    if len(refs) == 4:
        pick_ref, sums_ref = refs[:2]
        energy = total(damped * field) + total(pick_ref[...] * spread_ref[...])
        sums_ref[...] = lanes_of([total(field * field), energy])
    own_ref[...] = spread_out(spread_ref[...], sel_ref[...]) + damped


def combine_kernel(own_ref, near_ref, far_ref, mid_ref, share_ref, image_ref, near_out, far_out, mid_out, back_ref):
    for k, block in enumerate(read_blocks(near_ref, far_ref, mid_ref)[::-1]):
        back_ref[:, k * GH : (k + 1) * GH] = block
    image = own_ref[...] + spread_out(back_ref[...], share_ref[...])
    image_ref[...] = image
    write_blocks(split(pick(image, share_ref[...])), near_out, far_out, mid_out)


def local_kernel(image_ref, map_ref, diagonal_ref, local_ref, sums_ref, sel_ref):
    fill_selector(map_ref, sel_ref, 0)
    image = image_ref[...]
    local_ref[...] = pick(image, sel_ref[...])
    square = image * image
    weighted = diagonal_ref[...] * square
    sums_ref[...] = lanes_of([0.0, 0.0, total(square), total(weighted)])


def final_kernel(
    own_ref, near_ref, far_ref, mid_ref, share_ref, field_ref, image_ref, sums_ref, solution_ref, residual_ref, back_ref
):
    for k, block in enumerate(read_blocks(near_ref, far_ref, mid_ref)[::-1]):
        back_ref[:, k * GH : (k + 1) * GH] = block
    second = own_ref[...] + spread_out(back_ref[...], share_ref[...])
    field, image = field_ref[:TR], image_ref[:TR]
    row = jnp.sum(sums_ref[...], axis=0)
    s0, s1, s2, s3 = (row[:, k : k + 1] for k in range(4))
    step0 = quotient(s0, s1)
    ratio = quotient(quotient(determinant(s0, s1, s2), s1), s1)
    grow = 1.0 + ratio
    curvature = grow * grow * s1 - 2.0 * step0 * grow * s2 + step0 * step0 * s3
    step1 = quotient(ratio * s0, curvature)
    along = step0 + step1 * grow
    solution_ref[...] = along * field - (step0 * step1) * image
    residual_ref[...] = field - along * image + (step0 * step1) * second[:TR]


MESSAGE = (VMEM((2, TP, GH), F32), VMEM((2, TP, GH), F32), VMEM((TP, GH), F32))
WIDE = VMEM((TP, PICKS), F32)
FACES = VMEM((TP, F), F32)
GHOSTS = VMEM((TP, SHARED), F32)
ROW = VMEM((1, GH), F32)


OWN_SELECTOR = VMEM((F, PICKS), BF16)
ANY = pl.ANY


def call(kernel, out_shape, *args, scratch=(), held=VMEM, last=VMEM, first=VMEM):
    spaces = [VMEM] * (len(args) - 1) + [last]
    args = [pltpu.with_memory_space_constraint(a, pltpu.HBM if m is ANY else held) for a, m in zip(args, spaces)]
    return pl.pallas_call(
        kernel,
        in_specs=[pl.BlockSpec(memory_space=m) for m in spaces],
        out_specs=tuple(pl.BlockSpec(memory_space=VMEM if at else first) for at in range(len(out_shape))),
        out_shape=out_shape,
        scratch_shapes=scratch,
        compiler_params=pltpu.CompilerParams(vmem_limit_bytes=16 * 1024 * 1024),
    )(*args)


def shards(
    right_side, element_matrix, face_map, share_index, share_count, face_mass, absorbing, impedance
):
    count = lax.axis_size(DOM)
    core, odd = place()
    chips = count // 2

    def swap(value, partner_of):
        pairs = []
        for i in range(count):
            c, b = divmod(i, 2)
            partner = partner_of(c)
            pairs.append((i, 2 * partner + b if 0 <= partner < chips else i ^ 1))
        return lax.ppermute(value, DOM, pairs)

    def exchange(near, far, mid, beside):
        got_far = swap(far, lambda c: ((c + 1) ^ 1) - 1)
        got_near = swap(near, lambda c: c ^ 1)
        got_near, got_far, beside = lax.optimization_barrier((got_near, got_far, beside()))
        onward = jnp.where(core == odd, got_near[1], got_far[1])
        pair = jnp.stack([mid, onward])
        got_mid = lax.ppermute(pair, DOM, [(i, i ^ 1) for i in range(count)])
        return (got_near, got_far, got_mid), beside

    *sent, share, padded, held_map, diagonal = call(
        send_kernel,
        MESSAGE + (VMEM((F, SHARED), BF16), FACES, VMEM((SIDES, E), jnp.int32), VMEM((1, F), F32)),
        share_count,
        right_side,
        share_index[0],
        face_map,
        face_mass.reshape(1, F),
        absorbing.reshape(1, F),
        impedance.reshape(1, F),
        held=pltpu.HBM,
    )

    def select():
        return call(
            select_kernel,
            (VMEM((SHARED, PICKS), BF16), WIDE, VMEM((E // 128, DOFS, DOFS, 128), F32)),
            held_map,
            padded,
            element_matrix,
            scratch=[OWN_SELECTOR, VMEM((DOFS, DOFS, E), BF16), pltpu.SemaphoreType.DMA],
            last=ANY,
        )

    got, (selector, local, matrix) = exchange(*sent, select)
    scratch = [GHOSTS, VMEM((DOFS, E), F32)]
    *sent, spread, picked = call(product_kernel, MESSAGE + (WIDE, WIDE), *got, selector, matrix, local, scratch=scratch)

    def own0():
        return call(own_kernel, (ROW, FACES), spread, held_map, padded, diagonal, picked, scratch=[OWN_SELECTOR])

    got, (sums0, own) = exchange(*sent, own0)
    image, *sent = call(combine_kernel, (FACES,) + MESSAGE, own, *got, share, scratch=[GHOSTS])

    def local1():
        return call(local_kernel, (WIDE, ROW), image, held_map, diagonal, scratch=[OWN_SELECTOR])

    got, (local, sums1) = exchange(*sent, local1)
    row, *sent, spread = call(
        product_kernel,
        (jax.ShapeDtypeStruct((count, 1, GH), F32),) + MESSAGE + (WIDE,),
        *got,
        selector,
        matrix,
        local,
        sums0,
        sums1,
        scratch=[WIDE] + scratch + [VMEM((count, 1, GH), F32), pltpu.SemaphoreType.DMA],
        first=ANY,
    )
    row = lax.all_to_all(row, DOM, 0, 0)

    def own1():
        return call(own_kernel, (FACES,), spread, held_map, image, diagonal, scratch=[OWN_SELECTOR])

    got, (own,) = exchange(*sent, own1)
    out = jax.ShapeDtypeStruct((TR, F), F32)
    return call(final_kernel, (out, out), own, *got, share, padded, image, row, scratch=[GHOSTS])


def solution(mesh):
    line = P(DOM)
    in_specs = (
        P(None, DOM),
        P(None, None, DOM),
        P(None, DOM),
        P(DOM, None, None),
        P(DOM, None),
        line,
        line,
        line,
    )
    out_specs = (P(None, DOM), P(None, DOM))
    return jax.shard_map(shards, mesh=mesh, in_specs=in_specs, out_specs=out_specs, check_vma=False)
```

```python
import jax
import jax.numpy as jnp
from jax import lax
from jax.experimental import pallas as pl
from jax.experimental.pallas import tpu as pltpu
from jax.sharding import PartitionSpec as P


DOM = "dom"
TR = 18
TP = 24
SIDES = 4
E = 512
F = 1024
GH = 128
NB = 4
SHARED = NB * GH
PICKS = SIDES * E
DOFS = SIDES * TR
F32 = jnp.float32
BF16 = jnp.bfloat16
VMEM = pltpu.VMEM


def upper(x):
    scaled = 65537.0 * x
    return scaled - (scaled - x)


def pieces(x):
    hi = upper(x)
    rest = x - hi
    mid = upper(rest)
    return jnp.concatenate([hi, mid, rest - mid], axis=0).astype(BF16)


def joined(y):
    rows = y.shape[0] // 3
    return y[:rows] + y[rows : 2 * rows] + y[2 * rows :]


def pick(x, selector):
    return joined(jnp.dot(pieces(x), selector, preferred_element_type=F32))


def spread_out(x, selector):
    return joined(
        lax.dot_general(pieces(x), selector, (((1,), (1,)), ((), ())), preferred_element_type=F32)
    )


def place():
    here = lax.axis_index(DOM).astype(jnp.int32)
    return here & 1, (here >> 1) & 1


def split(x):
    return [x[:, k * GH : (k + 1) * GH] for k in range(NB)]


def write_blocks(blocks, near_ref, far_ref, mid_ref):
    core, odd = place()
    ahead, next_up, next_down, behind = (blocks[k] for k in (3, 2, 1, 0))
    near_ref[0] = jnp.where(odd == 1, behind, ahead)
    near_ref[1] = jnp.where(odd == 1, next_down, next_up)
    far_ref[0] = jnp.where(odd == 1, ahead, behind)
    far_ref[1] = jnp.where(odd == 1, next_up, next_down)
    mid_ref[...] = jnp.where(core == 1, next_down, next_up)


def read_blocks(near_ref, far_ref, mid_ref):
    core, odd = place()
    near, far, first, second = near_ref[0], far_ref[0], mid_ref[0], mid_ref[1]
    return [
        jnp.where(odd == 1, far, near),
        jnp.where(core == 1, second, first),
        jnp.where(core == 1, first, second),
        jnp.where(odd == 1, near, far),
    ]


def quotient(a, b):
    q = a / b
    return q + (a - q * b) / b


def exact_product(a, b):
    def halves(x):
        scaled = 4097.0 * x
        high = scaled - (scaled - x)
        return high, x - high

    product = a * b
    (ah, al), (bh, bl) = halves(a), halves(b)
    return product, ((ah * bh - product) + ah * bl + al * bh) + al * bl


def determinant(a, b, c):
    (first, first_rest), (second, second_rest) = exact_product(a, c), exact_product(b, b)
    return (first - second) + (first_rest - second_rest)


def lanes_of(values):
    lane = lax.broadcasted_iota(jnp.int32, (1, GH), 1)
    row = jnp.zeros((1, GH), F32)
    for at, value in enumerate(values):
        row = row + jnp.where(lane == at, value, 0.0)
    return row


def total(x):
    folded = sum(x[:, at : at + 128] for at in range(0, x.shape[1], 128))
    folded = sum(folded[at : at + 8] for at in range(0, x.shape[0], 8))
    return jnp.sum(jnp.sum(folded, axis=0, keepdims=True), axis=1, keepdims=True)


def send_kernel(count_ref, field_ref, index_ref, map_ref, mass_ref, absorbing_ref, impedance_ref, *refs):
    near_ref, far_ref, mid_ref, share_ref, padded_ref, map_out, diagonal_ref = refs
    for k in range(NB):
        rows = lax.broadcasted_iota(jnp.int32, (F, GH), 0)
        lanes = lax.broadcasted_iota(jnp.int32, (1, GH), 1)
        face = jnp.where(lanes < count_ref[:, k : k + 1], index_ref[k : k + 1, :], -1)
        share_ref[:, k * GH : (k + 1) * GH] = jnp.where(rows == face, 1.0, 0.0).astype(BF16)
    padded_ref[TR:, :] = jnp.zeros((TP - TR, F), F32)
    padded_ref[:TR, :] = field_ref[...]
    write_blocks(split(pick(padded_ref[...], share_ref[...])), near_ref, far_ref, mid_ref)
    map_out[...] = map_ref[...]
    diagonal_ref[...] = mass_ref[...] + absorbing_ref[...].astype(F32) * impedance_ref[...]


def fill_selector(map_ref, sel_ref, first):
    slots = sel_ref.shape[0]
    for s in range(SIDES):
        rows = lax.broadcasted_iota(jnp.int32, (slots, E), 0) + first
        sel_ref[:, s * E : (s + 1) * E] = jnp.where(rows == map_ref[s : s + 1, :], 1.0, 0.0).astype(BF16)


def select_kernel(map_ref, field_ref, matrix_ref, ghost_sel_ref, local_ref, wide_ref, sel_ref, held_ref, sem):
    copy = pltpu.make_async_copy(matrix_ref, held_ref, sem)
    copy.start()
    fill_selector(map_ref, sel_ref, 0)
    local_ref[...] = pick(field_ref[...], sel_ref[...])
    fill_selector(map_ref, ghost_sel_ref, F)
    copy.wait()
    for j in range(DOFS):
        for t in range(E // 128):
            wide_ref[t, j] = held_ref[j, :, t * 128 : (t + 1) * 128].astype(F32)


def product_kernel(near_ref, far_ref, mid_ref, sel_ref, matrix_ref, local_ref, *refs):
    last = len(refs) > 7
    near_out, far_out, mid_out, spread_ref, pick_ref, ghost_ref, prod_ref = refs[3:10] if last else refs
    for k, block in enumerate(read_blocks(near_ref, far_ref, mid_ref)):
        ghost_ref[:, k * GH : (k + 1) * GH] = block
    pick_ref[...] = local_ref[...] + pick(ghost_ref[...], sel_ref[...])
    for t in range(E // 128):
        acc = jnp.zeros((DOFS, 128), F32)
        for j in range(DOFS):
            s, c = divmod(j, TR)
            row = pick_ref[c : c + 1, s * E + t * 128 : s * E + (t + 1) * 128]
            acc = acc + matrix_ref[t, j] * row
        prod_ref[:, t * 128 : (t + 1) * 128] = acc
    spread_ref[TR:, :] = jnp.zeros((TP - TR, PICKS), F32)
    for s in range(SIDES):
        spread_ref[:TR, s * E : (s + 1) * E] = prod_ref[s * TR : (s + 1) * TR, :]
    if last:
        first_ref, second_ref, row_out = refs[:3]
        row_ref, sem = refs[10:]
        lane = lax.broadcasted_iota(jnp.int32, (1, GH), 1)
        energy = total(spread_ref[...] * pick_ref[...])
        row = first_ref[...] + second_ref[...] + jnp.where(lane == 3, energy, 0.0)
        row_ref[...] = jnp.broadcast_to(row[None], row_ref.shape)
        copy = pltpu.make_async_copy(row_ref, row_out, sem)
        copy.start()

    def send_back():
        parts = split(spread_out(spread_ref[...], sel_ref[...]))
        write_blocks(parts[::-1], near_out, far_out, mid_out)

    if last:
        pl.when(lax.axis_index(DOM) >= 0)(send_back)
        copy.wait()
    else:
        send_back()


def own_kernel(spread_ref, map_ref, field_ref, diagonal_ref, *refs):
    own_ref, sel_ref = refs[-2:]
    fill_selector(map_ref, sel_ref, 0)
    field = field_ref[...]
    damped = diagonal_ref[...] * field
    if len(refs) == 4:
        pick_ref, sums_ref = refs[:2]
        energy = total(damped * field) + total(pick_ref[...] * spread_ref[...])
        sums_ref[...] = lanes_of([total(field * field), energy])
    own_ref[...] = spread_out(spread_ref[...], sel_ref[...]) + damped


def combine_kernel(own_ref, near_ref, far_ref, mid_ref, share_ref, image_ref, near_out, far_out, mid_out, back_ref):
    for k, block in enumerate(read_blocks(near_ref, far_ref, mid_ref)[::-1]):
        back_ref[:, k * GH : (k + 1) * GH] = block
    image = own_ref[...] + spread_out(back_ref[...], share_ref[...])
    image_ref[...] = image
    write_blocks(split(pick(image, share_ref[...])), near_out, far_out, mid_out)


def local_kernel(image_ref, map_ref, diagonal_ref, local_ref, sums_ref, sel_ref):
    fill_selector(map_ref, sel_ref, 0)
    image = image_ref[...]
    local_ref[...] = pick(image, sel_ref[...])
    square = image * image
    weighted = diagonal_ref[...] * square
    sums_ref[...] = lanes_of([0.0, 0.0, total(square), total(weighted)])


def final_kernel(
    own_ref, near_ref, far_ref, mid_ref, share_ref, field_ref, image_ref, sums_ref, solution_ref, residual_ref, back_ref
):
    for k, block in enumerate(read_blocks(near_ref, far_ref, mid_ref)[::-1]):
        back_ref[:, k * GH : (k + 1) * GH] = block
    second = own_ref[...] + spread_out(back_ref[...], share_ref[...])
    field, image = field_ref[:TR], image_ref[:TR]
    row = jnp.sum(sums_ref[...], axis=0)
    s0, s1, s2, s3 = (row[:, k : k + 1] for k in range(4))
    step0 = quotient(s0, s1)
    ratio = quotient(quotient(determinant(s0, s1, s2), s1), s1)
    grow = 1.0 + ratio
    curvature = grow * grow * s1 - 2.0 * step0 * grow * s2 + step0 * step0 * s3
    step1 = quotient(ratio * s0, curvature)
    along = step0 + step1 * grow
    solution_ref[...] = along * field - (step0 * step1) * image
    residual_ref[...] = field - along * image + (step0 * step1) * second[:TR]


MESSAGE = (VMEM((2, TP, GH), F32), VMEM((2, TP, GH), F32), VMEM((TP, GH), F32))
WIDE = VMEM((TP, PICKS), F32)
FACES = VMEM((TP, F), F32)
GHOSTS = VMEM((TP, SHARED), F32)
ROW = VMEM((1, GH), F32)


OWN_SELECTOR = VMEM((F, PICKS), BF16)
ANY = pl.ANY


def call(kernel, out_shape, *args, scratch=(), held=VMEM, last=VMEM, first=VMEM):
    spaces = [VMEM] * (len(args) - 1) + [last]
    args = [pltpu.with_memory_space_constraint(a, pltpu.HBM if m is ANY else held) for a, m in zip(args, spaces)]
    return pl.pallas_call(
        kernel,
        in_specs=[pl.BlockSpec(memory_space=m) for m in spaces],
        out_specs=tuple(pl.BlockSpec(memory_space=VMEM if at else first) for at in range(len(out_shape))),
        out_shape=out_shape,
        scratch_shapes=scratch,
        compiler_params=pltpu.CompilerParams(vmem_limit_bytes=16 * 1024 * 1024),
    )(*args)


def shards(
    right_side, element_matrix, face_map, share_index, share_count, face_mass, absorbing, impedance
):
    count = lax.axis_size(DOM)
    core, odd = place()
    chips = count // 2

    def swap(value, partner_of):
        pairs = []
        for i in range(count):
            c, b = divmod(i, 2)
            partner = partner_of(c)
            pairs.append((i, 2 * partner + b if 0 <= partner < chips else i ^ 1))
        return lax.ppermute(value, DOM, pairs)

    def exchange(near, far, mid, beside):
        got_far = swap(far, lambda c: ((c + 1) ^ 1) - 1)
        got_near = swap(near, lambda c: c ^ 1)
        got_near, got_far, beside = lax.optimization_barrier((got_near, got_far, beside()))
        onward = jnp.where(core == odd, got_near[1], got_far[1])
        pair = jnp.stack([mid, onward])
        got_mid = lax.ppermute(pair, DOM, [(i, i ^ 1) for i in range(count)])
        return (got_near, got_far, got_mid), beside

    *sent, share, padded, held_map, diagonal = call(
        send_kernel,
        MESSAGE + (VMEM((F, SHARED), BF16), FACES, VMEM((SIDES, E), jnp.int32), VMEM((1, F), F32)),
        share_count,
        right_side,
        share_index[0],
        face_map,
        face_mass.reshape(1, F),
        absorbing.reshape(1, F),
        impedance.reshape(1, F),
        held=pltpu.HBM,
    )

    def select():
        return call(
            select_kernel,
            (VMEM((SHARED, PICKS), BF16), WIDE, VMEM((E // 128, DOFS, DOFS, 128), F32)),
            held_map,
            padded,
            element_matrix,
            scratch=[OWN_SELECTOR, VMEM((DOFS, DOFS, E), BF16), pltpu.SemaphoreType.DMA],
            last=ANY,
        )

    got, (selector, local, matrix) = exchange(*sent, select)
    scratch = [GHOSTS, VMEM((DOFS, E), F32)]
    *sent, spread, picked = call(product_kernel, MESSAGE + (WIDE, WIDE), *got, selector, matrix, local, scratch=scratch)

    def own0():
        return call(own_kernel, (ROW, FACES), spread, held_map, padded, diagonal, picked, scratch=[OWN_SELECTOR])

    got, (sums0, own) = exchange(*sent, own0)
    image, *sent = call(combine_kernel, (FACES,) + MESSAGE, own, *got, share, scratch=[GHOSTS])

    def local1():
        return call(local_kernel, (WIDE, ROW), image, held_map, diagonal, scratch=[OWN_SELECTOR])

    got, (local, sums1) = exchange(*sent, local1)
    row, *sent, spread = call(
        product_kernel,
        (jax.ShapeDtypeStruct((count, 1, GH), F32),) + MESSAGE + (WIDE,),
        *got,
        selector,
        matrix,
        local,
        sums0,
        sums1,
        scratch=[WIDE] + scratch + [VMEM((count, 1, GH), F32), pltpu.SemaphoreType.DMA],
        first=ANY,
    )
    row = lax.all_to_all(row, DOM, 0, 0)

    def own1():
        return call(own_kernel, (FACES,), spread, held_map, image, diagonal, scratch=[OWN_SELECTOR])

    got, (own,) = exchange(*sent, own1)
    out = jax.ShapeDtypeStruct((TR, F), F32)
    return call(final_kernel, (out, out), own, *got, share, padded, image, row, scratch=[GHOSTS])


def solution(mesh):
    line = P(DOM)
    in_specs = (
        P(None, DOM),
        P(None, None, DOM),
        P(None, DOM),
        P(DOM, None, None),
        P(DOM, None),
        line,
        line,
        line,
    )
    out_specs = (P(None, DOM), P(None, DOM))
    return jax.shard_map(shards, mesh=mesh, in_specs=in_specs, out_specs=out_specs, check_vma=False)
```

```python
import jax
import jax.numpy as jnp
from jax import lax
from jax.experimental import pallas as pl
from jax.experimental.pallas import tpu as pltpu
from jax.sharding import PartitionSpec as P


DOM = "dom"
TR = 18
TP = 24
SIDES = 4
E = 512
F = 1024
GH = 128
NB = 4
SHARED = NB * GH
PICKS = SIDES * E
DOFS = SIDES * TR
F32 = jnp.float32
BF16 = jnp.bfloat16
VMEM = pltpu.VMEM


def upper(x):
    scaled = 65537.0 * x
    return scaled - (scaled - x)


def pieces(x):
    hi = upper(x)
    return jnp.concatenate([hi, x - hi], axis=0).astype(BF16)


def joined(y):
    rows = y.shape[0] // 2
    return y[:rows] + y[rows:]


def pick(x, selector):
    return joined(jnp.dot(pieces(x), selector, preferred_element_type=F32))


def spread_out(x, selector):
    return joined(
        lax.dot_general(pieces(x), selector, (((1,), (1,)), ((), ())), preferred_element_type=F32)
    )


def place():
    here = lax.axis_index(DOM).astype(jnp.int32)
    return here & 1, (here >> 1) & 1


def split(x):
    return [x[:, k * GH : (k + 1) * GH] for k in range(NB)]


def write_blocks(blocks, near_ref, far_ref, mid_ref):
    core, odd = place()
    ahead, next_up, next_down, behind = (blocks[k] for k in (3, 2, 1, 0))
    near_ref[0] = jnp.where(odd == 1, behind, ahead)
    near_ref[1] = jnp.where(odd == 1, next_down, next_up)
    far_ref[0] = jnp.where(odd == 1, ahead, behind)
    far_ref[1] = jnp.where(odd == 1, next_up, next_down)
    mid_ref[...] = jnp.where(core == 1, next_down, next_up)


def read_blocks(near_ref, far_ref, mid_ref):
    core, odd = place()
    near, far, first, second = near_ref[0], far_ref[0], mid_ref[0], mid_ref[1]
    return [
        jnp.where(odd == 1, far, near),
        jnp.where(core == 1, second, first),
        jnp.where(core == 1, first, second),
        jnp.where(odd == 1, near, far),
    ]


def quotient(a, b):
    q = a / b
    return q + (a - q * b) / b


def exact_product(a, b):
    def halves(x):
        scaled = 4097.0 * x
        high = scaled - (scaled - x)
        return high, x - high

    product = a * b
    (ah, al), (bh, bl) = halves(a), halves(b)
    return product, ((ah * bh - product) + ah * bl + al * bh) + al * bl


def determinant(a, b, c):
    (first, first_rest), (second, second_rest) = exact_product(a, c), exact_product(b, b)
    return (first - second) + (first_rest - second_rest)


def lanes_of(values):
    lane = lax.broadcasted_iota(jnp.int32, (1, GH), 1)
    row = jnp.zeros((1, GH), F32)
    for at, value in enumerate(values):
        row = row + jnp.where(lane == at, value, 0.0)
    return row


def total(x):
    folded = sum(x[:, at : at + 128] for at in range(0, x.shape[1], 128))
    folded = sum(folded[at : at + 8] for at in range(0, x.shape[0], 8))
    return jnp.sum(jnp.sum(folded, axis=0, keepdims=True), axis=1, keepdims=True)


def send_kernel(count_ref, field_ref, index_ref, map_ref, mass_ref, absorbing_ref, impedance_ref, *refs):
    near_ref, far_ref, mid_ref, share_ref, padded_ref, map_out, diagonal_ref = refs
    for k in range(NB):
        rows = lax.broadcasted_iota(jnp.int32, (F, GH), 0)
        lanes = lax.broadcasted_iota(jnp.int32, (1, GH), 1)
        face = jnp.where(lanes < count_ref[:, k : k + 1], index_ref[k : k + 1, :], -1)
        share_ref[:, k * GH : (k + 1) * GH] = jnp.where(rows == face, 1.0, 0.0).astype(BF16)
    padded_ref[TR:, :] = jnp.zeros((TP - TR, F), F32)
    padded_ref[:TR, :] = field_ref[...]
    write_blocks(split(pick(padded_ref[...], share_ref[...])), near_ref, far_ref, mid_ref)
    map_out[...] = map_ref[...]
    diagonal_ref[...] = mass_ref[...] + absorbing_ref[...].astype(F32) * impedance_ref[...]


def fill_selector(map_ref, sel_ref, first):
    slots = sel_ref.shape[0]
    for s in range(SIDES):
        rows = lax.broadcasted_iota(jnp.int32, (slots, E), 0) + first
        sel_ref[:, s * E : (s + 1) * E] = jnp.where(rows == map_ref[s : s + 1, :], 1.0, 0.0).astype(BF16)


def select_kernel(map_ref, field_ref, matrix_ref, ghost_sel_ref, local_ref, wide_ref, sel_ref, held_ref, sem):
    copy = pltpu.make_async_copy(matrix_ref, held_ref, sem)
    copy.start()
    fill_selector(map_ref, sel_ref, 0)
    local_ref[...] = pick(field_ref[...], sel_ref[...])
    fill_selector(map_ref, ghost_sel_ref, F)
    copy.wait()
    for j in range(DOFS):
        for t in range(E // 128):
            wide_ref[t, j] = held_ref[j, :, t * 128 : (t + 1) * 128].astype(F32)


def product_kernel(near_ref, far_ref, mid_ref, sel_ref, matrix_ref, local_ref, *refs):
    last = len(refs) > 7
    near_out, far_out, mid_out, spread_ref, pick_ref, ghost_ref, prod_ref = refs[3:10] if last else refs
    for k, block in enumerate(read_blocks(near_ref, far_ref, mid_ref)):
        ghost_ref[:, k * GH : (k + 1) * GH] = block
    pick_ref[...] = local_ref[...] + pick(ghost_ref[...], sel_ref[...])
    for t in range(E // 128):
        acc = jnp.zeros((DOFS, 128), F32)
        for j in range(DOFS):
            s, c = divmod(j, TR)
            row = pick_ref[c : c + 1, s * E + t * 128 : s * E + (t + 1) * 128]
            acc = acc + matrix_ref[t, j] * row
        prod_ref[:, t * 128 : (t + 1) * 128] = acc
    spread_ref[TR:, :] = jnp.zeros((TP - TR, PICKS), F32)
    for s in range(SIDES):
        spread_ref[:TR, s * E : (s + 1) * E] = prod_ref[s * TR : (s + 1) * TR, :]
    if last:
        first_ref, second_ref, row_out = refs[:3]
        row_ref, sem = refs[10:]
        lane = lax.broadcasted_iota(jnp.int32, (1, GH), 1)
        energy = total(spread_ref[...] * pick_ref[...])
        row = first_ref[...] + second_ref[...] + jnp.where(lane == 3, energy, 0.0)
        row_ref[...] = jnp.broadcast_to(row[None], row_ref.shape)
        copy = pltpu.make_async_copy(row_ref, row_out, sem)
        copy.start()

    def send_back():
        parts = split(spread_out(spread_ref[...], sel_ref[...]))
        write_blocks(parts[::-1], near_out, far_out, mid_out)

    if last:
        pl.when(lax.axis_index(DOM) >= 0)(send_back)
        copy.wait()
    else:
        send_back()


def own_kernel(spread_ref, map_ref, field_ref, diagonal_ref, *refs):
    own_ref, sel_ref = refs[-2:]
    fill_selector(map_ref, sel_ref, 0)
    field = field_ref[...]
    damped = diagonal_ref[...] * field
    if len(refs) == 4:
        pick_ref, sums_ref = refs[:2]
        energy = total(damped * field) + total(pick_ref[...] * spread_ref[...])
        sums_ref[...] = lanes_of([total(field * field), energy])
    own_ref[...] = spread_out(spread_ref[...], sel_ref[...]) + damped


def combine_kernel(own_ref, near_ref, far_ref, mid_ref, share_ref, image_ref, near_out, far_out, mid_out, back_ref):
    for k, block in enumerate(read_blocks(near_ref, far_ref, mid_ref)[::-1]):
        back_ref[:, k * GH : (k + 1) * GH] = block
    image = own_ref[...] + spread_out(back_ref[...], share_ref[...])
    image_ref[...] = image
    write_blocks(split(pick(image, share_ref[...])), near_out, far_out, mid_out)


def local_kernel(image_ref, map_ref, diagonal_ref, local_ref, sums_ref, sel_ref):
    fill_selector(map_ref, sel_ref, 0)
    image = image_ref[...]
    local_ref[...] = pick(image, sel_ref[...])
    square = image * image
    weighted = diagonal_ref[...] * square
    sums_ref[...] = lanes_of([0.0, 0.0, total(square), total(weighted)])


def final_kernel(
    own_ref, near_ref, far_ref, mid_ref, share_ref, field_ref, image_ref, sums_ref, solution_ref, residual_ref, back_ref
):
    for k, block in enumerate(read_blocks(near_ref, far_ref, mid_ref)[::-1]):
        back_ref[:, k * GH : (k + 1) * GH] = block
    second = own_ref[...] + spread_out(back_ref[...], share_ref[...])
    field, image = field_ref[:TR], image_ref[:TR]
    row = sums_ref[...]
    while row.shape[0] > 1:
        half = row.shape[0] // 2
        row = row[:half] + row[half:]
    row = row[0]
    s0, s1, s2, s3 = (row[:, k : k + 1] for k in range(4))
    step0 = quotient(s0, s1)
    ratio = quotient(quotient(determinant(s0, s1, s2), s1), s1)
    grow = 1.0 + ratio
    curvature = grow * grow * s1 - 2.0 * step0 * grow * s2 + step0 * step0 * s3
    step1 = quotient(ratio * s0, curvature)
    along = step0 + step1 * grow
    solution_ref[...] = along * field - (step0 * step1) * image
    residual_ref[...] = field - along * image + (step0 * step1) * second[:TR]


MESSAGE = (VMEM((2, TP, GH), F32), VMEM((2, TP, GH), F32), VMEM((TP, GH), F32))
WIDE = VMEM((TP, PICKS), F32)
FACES = VMEM((TP, F), F32)
GHOSTS = VMEM((TP, SHARED), F32)
ROW = VMEM((1, GH), F32)


OWN_SELECTOR = VMEM((F, PICKS), BF16)
ANY = pl.ANY


def call(kernel, out_shape, *args, scratch=(), held=VMEM, last=VMEM, first=VMEM):
    spaces = [VMEM] * (len(args) - 1) + [last]
    args = [pltpu.with_memory_space_constraint(a, pltpu.HBM if m is ANY else held) for a, m in zip(args, spaces)]
    return pl.pallas_call(
        kernel,
        in_specs=[pl.BlockSpec(memory_space=m) for m in spaces],
        out_specs=tuple(pl.BlockSpec(memory_space=VMEM if at else first) for at in range(len(out_shape))),
        out_shape=out_shape,
        scratch_shapes=scratch,
        compiler_params=pltpu.CompilerParams(vmem_limit_bytes=16 * 1024 * 1024),
    )(*args)


def shards(
    right_side, element_matrix, face_map, share_index, share_count, face_mass, absorbing, impedance
):
    count = lax.axis_size(DOM)
    core, odd = place()
    chips = count // 2

    def swap(value, partner_of):
        pairs = []
        for i in range(count):
            c, b = divmod(i, 2)
            partner = partner_of(c)
            pairs.append((i, 2 * partner + b if 0 <= partner < chips else i ^ 1))
        return lax.ppermute(value, DOM, pairs)

    def exchange(near, far, mid, beside):
        got_far = swap(far, lambda c: ((c + 1) ^ 1) - 1)
        got_near = swap(near, lambda c: c ^ 1)
        got_near, got_far, beside = lax.optimization_barrier((got_near, got_far, beside()))
        onward = jnp.where(core == odd, got_near[1], got_far[1])
        pair = jnp.stack([mid, onward])
        got_mid = lax.ppermute(pair, DOM, [(i, i ^ 1) for i in range(count)])
        return (got_near, got_far, got_mid), beside

    *sent, share, padded, held_map, diagonal = call(
        send_kernel,
        MESSAGE + (VMEM((F, SHARED), BF16), FACES, VMEM((SIDES, E), jnp.int32), VMEM((1, F), F32)),
        share_count,
        right_side,
        share_index[0],
        face_map,
        face_mass.reshape(1, F),
        absorbing.reshape(1, F),
        impedance.reshape(1, F),
        held=pltpu.HBM,
    )

    def select():
        return call(
            select_kernel,
            (VMEM((SHARED, PICKS), BF16), WIDE, VMEM((E // 128, DOFS, DOFS, 128), F32)),
            held_map,
            padded,
            element_matrix,
            scratch=[OWN_SELECTOR, VMEM((DOFS, DOFS, E), BF16), pltpu.SemaphoreType.DMA],
            last=ANY,
        )

    got, (selector, local, matrix) = exchange(*sent, select)
    scratch = [GHOSTS, VMEM((DOFS, E), F32)]
    *sent, spread, picked = call(product_kernel, MESSAGE + (WIDE, WIDE), *got, selector, matrix, local, scratch=scratch)

    def own0():
        return call(own_kernel, (ROW, FACES), spread, held_map, padded, diagonal, picked, scratch=[OWN_SELECTOR])

    got, (sums0, own) = exchange(*sent, own0)
    image, *sent = call(combine_kernel, (FACES,) + MESSAGE, own, *got, share, scratch=[GHOSTS])

    def local1():
        return call(local_kernel, (WIDE, ROW), image, held_map, diagonal, scratch=[OWN_SELECTOR])

    got, (local, sums1) = exchange(*sent, local1)
    row, *sent, spread = call(
        product_kernel,
        (jax.ShapeDtypeStruct((count, 1, GH), F32),) + MESSAGE + (WIDE,),
        *got,
        selector,
        matrix,
        local,
        sums0,
        sums1,
        scratch=[WIDE] + scratch + [VMEM((count, 1, GH), F32), pltpu.SemaphoreType.DMA],
        first=ANY,
    )
    row = lax.all_to_all(row, DOM, 0, 0)

    def own1():
        return call(own_kernel, (FACES,), spread, held_map, image, diagonal, scratch=[OWN_SELECTOR])

    got, (own,) = exchange(*sent, own1)
    out = jax.ShapeDtypeStruct((TR, F), F32)
    return call(final_kernel, (out, out), own, *got, share, padded, image, row, scratch=[GHOSTS])


def solution(mesh):
    line = P(DOM)
    in_specs = (
        P(None, DOM),
        P(None, None, DOM),
        P(None, DOM),
        P(DOM, None, None),
        P(DOM, None),
        line,
        line,
        line,
    )
    out_specs = (P(None, DOM), P(None, DOM))
    return jax.shard_map(shards, mesh=mesh, in_specs=in_specs, out_specs=out_specs, check_vma=False)
```

```python
import jax
import jax.numpy as jnp
from jax import lax
from jax.experimental import pallas as pl
from jax.experimental.pallas import tpu as pltpu
from jax.sharding import PartitionSpec as P


DOM = "dom"
TR = 18
TP = 24
SIDES = 4
E = 512
F = 1024
GH = 128
NB = 4
SHARED = NB * GH
PICKS = SIDES * E
DOFS = SIDES * TR
F32 = jnp.float32
BF16 = jnp.bfloat16
VMEM = pltpu.VMEM


def upper(x):
    scaled = 65537.0 * x
    return scaled - (scaled - x)


def pieces(x):
    hi = upper(x)
    return jnp.concatenate([hi, x - hi], axis=0).astype(BF16)


def joined(y):
    rows = y.shape[0] // 2
    return y[:rows] + y[rows:]


def pick(x, selector):
    return joined(jnp.dot(pieces(x), selector, preferred_element_type=F32))


def spread_out(x, selector):
    return joined(
        lax.dot_general(pieces(x), selector, (((1,), (1,)), ((), ())), preferred_element_type=F32)
    )


def place():
    here = lax.axis_index(DOM).astype(jnp.int32)
    return here & 1, (here >> 1) & 1


def split(x):
    return [x[:, k * GH : (k + 1) * GH] for k in range(NB)]


def write_blocks(blocks, near_ref, far_ref, mid_ref):
    core, odd = place()
    ahead, next_up, next_down, behind = (blocks[k] for k in (3, 2, 1, 0))
    near_ref[:TR] = jnp.where(odd == 1, behind, ahead)[:TR]
    near_ref[TR : 2 * TR] = jnp.where(odd == 1, next_down, next_up)[:TR]
    far_ref[:TR] = jnp.where(odd == 1, ahead, behind)[:TR]
    far_ref[TR : 2 * TR] = jnp.where(odd == 1, next_up, next_down)[:TR]
    mid_ref[...] = jnp.where(core == 1, next_down, next_up)


def read_blocks(near_ref, far_ref, mid_ref):
    core, odd = place()
    near, far, first, second = near_ref[:TR], far_ref[:TR], mid_ref[0, :TR], mid_ref[1, :TR]
    return [
        jnp.where(odd == 1, far, near),
        jnp.where(core == 1, second, first),
        jnp.where(core == 1, first, second),
        jnp.where(odd == 1, near, far),
    ]


def quotient(a, b):
    q = a / b
    return q + (a - q * b) / b


def exact_product(a, b):
    def halves(x):
        scaled = 4097.0 * x
        high = scaled - (scaled - x)
        return high, x - high

    product = a * b
    (ah, al), (bh, bl) = halves(a), halves(b)
    return product, ((ah * bh - product) + ah * bl + al * bh) + al * bl


def determinant(a, b, c):
    (first, first_rest), (second, second_rest) = exact_product(a, c), exact_product(b, b)
    return (first - second) + (first_rest - second_rest)


def lanes_of(values):
    lane = lax.broadcasted_iota(jnp.int32, (1, GH), 1)
    row = jnp.zeros((1, GH), F32)
    for at, value in enumerate(values):
        row = row + jnp.where(lane == at, value, 0.0)
    return row


def total(x):
    folded = sum(x[:, at : at + 128] for at in range(0, x.shape[1], 128))
    folded = sum(folded[at : at + 8] for at in range(0, x.shape[0], 8))
    return jnp.sum(jnp.sum(folded, axis=0, keepdims=True), axis=1, keepdims=True)


def send_kernel(count_ref, field_ref, index_ref, map_ref, mass_ref, absorbing_ref, impedance_ref, *refs):
    near_ref, far_ref, mid_ref, share_ref, padded_ref, map_out, diagonal_ref = refs
    for k in range(NB):
        rows = lax.broadcasted_iota(jnp.int32, (F, GH), 0)
        lanes = lax.broadcasted_iota(jnp.int32, (1, GH), 1)
        face = jnp.where(lanes < count_ref[:, k : k + 1], index_ref[k : k + 1, :], -1)
        share_ref[:, k * GH : (k + 1) * GH] = jnp.where(rows == face, 1.0, 0.0).astype(BF16)
    padded_ref[TR:, :] = jnp.zeros((TP - TR, F), F32)
    padded_ref[:TR, :] = field_ref[...]
    write_blocks(split(pick(padded_ref[...], share_ref[...])), near_ref, far_ref, mid_ref)
    map_out[...] = map_ref[...]
    diagonal_ref[...] = mass_ref[...] + absorbing_ref[...].astype(F32) * impedance_ref[...]


def fill_selector(map_ref, sel_ref, first):
    slots = sel_ref.shape[0]
    for s in range(SIDES):
        rows = lax.broadcasted_iota(jnp.int32, (slots, E), 0) + first
        sel_ref[:, s * E : (s + 1) * E] = jnp.where(rows == map_ref[s : s + 1, :], 1.0, 0.0).astype(BF16)


def select_kernel(map_ref, field_ref, matrix_ref, ghost_sel_ref, local_ref, wide_ref, sel_ref, held_ref, sem):
    copy = pltpu.make_async_copy(matrix_ref, held_ref, sem)
    copy.start()
    fill_selector(map_ref, sel_ref, 0)
    local_ref[...] = pick(field_ref[...], sel_ref[...])
    fill_selector(map_ref, ghost_sel_ref, F)
    copy.wait()
    for j in range(DOFS):
        for t in range(E // 128):
            wide_ref[t, j] = held_ref[j, :, t * 128 : (t + 1) * 128].astype(F32)


def product_kernel(near_ref, far_ref, mid_ref, sel_ref, matrix_ref, local_ref, *refs):
    last = len(refs) > 7
    near_out, far_out, mid_out, spread_ref, pick_ref, ghost_ref, prod_ref = refs[3:10] if last else refs
    ghost_ref[TR:, :] = jnp.zeros((TP - TR, SHARED), F32)
    for k, block in enumerate(read_blocks(near_ref, far_ref, mid_ref)):
        ghost_ref[:TR, k * GH : (k + 1) * GH] = block
    pick_ref[...] = local_ref[...] + pick(ghost_ref[...], sel_ref[...])
    for t in range(E // 128):
        acc = jnp.zeros((DOFS, 128), F32)
        for j in range(DOFS):
            s, c = divmod(j, TR)
            row = pick_ref[c : c + 1, s * E + t * 128 : s * E + (t + 1) * 128]
            acc = acc + matrix_ref[t, j] * row
        prod_ref[:, t * 128 : (t + 1) * 128] = acc
    spread_ref[TR:, :] = jnp.zeros((TP - TR, PICKS), F32)
    for s in range(SIDES):
        spread_ref[:TR, s * E : (s + 1) * E] = prod_ref[s * TR : (s + 1) * TR, :]
    if last:
        first_ref, second_ref, row_out = refs[:3]
        row_ref, sem = refs[10:]
        lane = lax.broadcasted_iota(jnp.int32, (1, GH), 1)
        energy = total(spread_ref[...] * pick_ref[...])
        row = first_ref[...] + second_ref[...] + jnp.where(lane == 3, energy, 0.0)
        row_ref[...] = jnp.broadcast_to(row[None], row_ref.shape)
        copy = pltpu.make_async_copy(row_ref, row_out, sem)
        copy.start()

    def send_back():
        parts = split(spread_out(spread_ref[...], sel_ref[...]))
        write_blocks(parts[::-1], near_out, far_out, mid_out)

    if last:
        pl.when(lax.axis_index(DOM) >= 0)(send_back)
        copy.wait()
    else:
        send_back()


def own_kernel(spread_ref, map_ref, field_ref, diagonal_ref, *refs):
    own_ref, sel_ref = refs[-2:]
    fill_selector(map_ref, sel_ref, 0)
    field = field_ref[...]
    damped = diagonal_ref[...] * field
    if len(refs) == 4:
        pick_ref, sums_ref = refs[:2]
        energy = total(damped * field) + total(pick_ref[...] * spread_ref[...])
        sums_ref[...] = lanes_of([total(field * field), energy])
    own_ref[...] = spread_out(spread_ref[...], sel_ref[...]) + damped


def combine_kernel(own_ref, near_ref, far_ref, mid_ref, share_ref, image_ref, near_out, far_out, mid_out, back_ref):
    back_ref[TR:, :] = jnp.zeros((TP - TR, SHARED), F32)
    for k, block in enumerate(read_blocks(near_ref, far_ref, mid_ref)[::-1]):
        back_ref[:TR, k * GH : (k + 1) * GH] = block
    image = own_ref[...] + spread_out(back_ref[...], share_ref[...])
    image_ref[...] = image
    write_blocks(split(pick(image, share_ref[...])), near_out, far_out, mid_out)


def local_kernel(image_ref, map_ref, diagonal_ref, local_ref, sums_ref, sel_ref):
    fill_selector(map_ref, sel_ref, 0)
    image = image_ref[...]
    local_ref[...] = pick(image, sel_ref[...])
    square = image * image
    weighted = diagonal_ref[...] * square
    sums_ref[...] = lanes_of([0.0, 0.0, total(square), total(weighted)])


def final_kernel(
    own_ref, near_ref, far_ref, mid_ref, share_ref, field_ref, image_ref, sums_ref, solution_ref, residual_ref, back_ref
):
    back_ref[TR:, :] = jnp.zeros((TP - TR, SHARED), F32)
    for k, block in enumerate(read_blocks(near_ref, far_ref, mid_ref)[::-1]):
        back_ref[:TR, k * GH : (k + 1) * GH] = block
    second = own_ref[...] + spread_out(back_ref[...], share_ref[...])
    field, image = field_ref[:TR], image_ref[:TR]
    row = sums_ref[...]
    while row.shape[0] > 1:
        half = row.shape[0] // 2
        row = row[:half] + row[half:]
    row = row[0]
    s0, s1, s2, s3 = (row[:, k : k + 1] for k in range(4))
    step0 = quotient(s0, s1)
    ratio = quotient(quotient(determinant(s0, s1, s2), s1), s1)
    grow = 1.0 + ratio
    curvature = grow * grow * s1 - 2.0 * step0 * grow * s2 + step0 * step0 * s3
    step1 = quotient(ratio * s0, curvature)
    along = step0 + step1 * grow
    solution_ref[...] = along * field - (step0 * step1) * image
    residual_ref[...] = field - along * image + (step0 * step1) * second[:TR]


MESSAGE = (VMEM((2 * TR, GH), F32), VMEM((2 * TR, GH), F32), VMEM((TP, GH), F32))
WIDE = VMEM((TP, PICKS), F32)
FACES = VMEM((TP, F), F32)
GHOSTS = VMEM((TP, SHARED), F32)
ROW = VMEM((1, GH), F32)


OWN_SELECTOR = VMEM((F, PICKS), BF16)
ANY = pl.ANY


def call(kernel, out_shape, *args, scratch=(), held=VMEM, last=VMEM, first=VMEM):
    spaces = [VMEM] * (len(args) - 1) + [last]
    args = [pltpu.with_memory_space_constraint(a, pltpu.HBM if m is ANY else held) for a, m in zip(args, spaces)]
    return pl.pallas_call(
        kernel,
        in_specs=[pl.BlockSpec(memory_space=m) for m in spaces],
        out_specs=tuple(pl.BlockSpec(memory_space=VMEM if at else first) for at in range(len(out_shape))),
        out_shape=out_shape,
        scratch_shapes=scratch,
        compiler_params=pltpu.CompilerParams(vmem_limit_bytes=16 * 1024 * 1024),
    )(*args)


def shards(
    right_side, element_matrix, face_map, share_index, share_count, face_mass, absorbing, impedance
):
    count = lax.axis_size(DOM)
    core, odd = place()
    chips = count // 2

    def swap(value, partner_of):
        pairs = []
        for i in range(count):
            c, b = divmod(i, 2)
            partner = partner_of(c)
            pairs.append((i, 2 * partner + b if 0 <= partner < chips else i ^ 1))
        return lax.ppermute(value, DOM, pairs)

    def exchange(near, far, mid, beside):
        got_far = swap(far, lambda c: ((c + 1) ^ 1) - 1)
        got_near = swap(near, lambda c: c ^ 1)
        got_near, got_far, beside = lax.optimization_barrier((got_near, got_far, beside()))
        onward = jnp.pad(jnp.where(core == odd, got_near, got_far)[TR:], ((0, TP - TR), (0, 0)))
        pair = jnp.stack([mid, onward])
        got_mid = lax.ppermute(pair, DOM, [(i, i ^ 1) for i in range(count)])
        return (got_near, got_far, got_mid), beside

    *sent, share, padded, held_map, diagonal = call(
        send_kernel,
        MESSAGE + (VMEM((F, SHARED), BF16), FACES, VMEM((SIDES, E), jnp.int32), VMEM((1, F), F32)),
        share_count,
        right_side,
        share_index[0],
        face_map,
        face_mass.reshape(1, F),
        absorbing.reshape(1, F),
        impedance.reshape(1, F),
        held=pltpu.HBM,
    )

    def select():
        return call(
            select_kernel,
            (VMEM((SHARED, PICKS), BF16), WIDE, VMEM((E // 128, DOFS, DOFS, 128), F32)),
            held_map,
            padded,
            element_matrix,
            scratch=[OWN_SELECTOR, VMEM((DOFS, DOFS, E), BF16), pltpu.SemaphoreType.DMA],
            last=ANY,
        )

    got, (selector, local, matrix) = exchange(*sent, select)
    scratch = [GHOSTS, VMEM((DOFS, E), F32)]
    *sent, spread, picked = call(product_kernel, MESSAGE + (WIDE, WIDE), *got, selector, matrix, local, scratch=scratch)

    def own0():
        return call(own_kernel, (ROW, FACES), spread, held_map, padded, diagonal, picked, scratch=[OWN_SELECTOR])

    got, (sums0, own) = exchange(*sent, own0)
    image, *sent = call(combine_kernel, (FACES,) + MESSAGE, own, *got, share, scratch=[GHOSTS])

    def local1():
        return call(local_kernel, (WIDE, ROW), image, held_map, diagonal, scratch=[OWN_SELECTOR])

    got, (local, sums1) = exchange(*sent, local1)
    row, *sent, spread = call(
        product_kernel,
        (jax.ShapeDtypeStruct((count, 1, GH), F32),) + MESSAGE + (WIDE,),
        *got,
        selector,
        matrix,
        local,
        sums0,
        sums1,
        scratch=[WIDE] + scratch + [VMEM((count, 1, GH), F32), pltpu.SemaphoreType.DMA],
        first=ANY,
    )
    row = lax.all_to_all(row, DOM, 0, 0)

    def own1():
        return call(own_kernel, (FACES,), spread, held_map, image, diagonal, scratch=[OWN_SELECTOR])

    got, (own,) = exchange(*sent, own1)
    out = jax.ShapeDtypeStruct((TR, F), F32)
    return call(final_kernel, (out, out), own, *got, share, padded, image, row, scratch=[GHOSTS])


def solution(mesh):
    line = P(DOM)
    in_specs = (
        P(None, DOM),
        P(None, None, DOM),
        P(None, DOM),
        P(DOM, None, None),
        P(DOM, None),
        line,
        line,
        line,
    )
    out_specs = (P(None, DOM), P(None, DOM))
    return jax.shard_map(shards, mesh=mesh, in_specs=in_specs, out_specs=out_specs, check_vma=False)
```
